512 devices in a mesh: dp: 4 (over x), expert: 128 (over y, z, core).
Axes of the slice: x: 4, y: 4, z: 16, core: 2. Of those that a mesh axis runs over, the one named last changes fastest.
Arguments:
- tokens: bfloat16 [49152, 2048], P(('dp', 'expert')), may hold values from -6 to 6
- routes: int32 [49152, 8], P(('dp', 'expert')), may hold values from 0 to 127, all different within a row; in each aligned block of 96 rows (0 to 95, 96 to 191, ...) at most 8 rows name the same one
- weights: bfloat16 [128, 2, 768, 2048], P('expert', None, 'dp'), may hold values from -0.125 to 0.125
- keep_mask: int32 [128, 2, 768, 128], P('expert', None, 'dp'), may hold values from 0 to 1, as said below
- inv_factor: float32 [128, 128, 2048], P('expert'), as said below
Outputs:
- hidden: bfloat16 [49152, 8, 768], P(('dp', 'expert'))
The draws below stay inside these ranges and needn't reach their ends.
Inputs may be any that keep to these rules, and one draw needn't show every extreme that they name: `routes`: each token names 8 different experts; the 96 rows of one device name any one expert at most 8 times. `keep_mask`: each row of 128 entries holds exactly 64 ones. `inv_factor`: each expert's factor is upper triangular: entry (i, j) is zero for j < i, and the diagonal entry (i, i) lies in [0.6, 1.6].
All inputs are finite; a program needn't handle non-finite values.
Results may differ from the reference program's by a relative error of at most 0.0058.
Values may be sent and summed in bfloat16 or wider, within the bound.
A program may use at most 64 MiB of HBM per device.

```python
import math
import jax
import jax.numpy as jnp
import numpy as np
from jax import lax

D = 2048
FW = 768
TOP = 8
BLOCK = 128
KEEP = 64
TOK_DEV = 96
EXPERTS = 128
CAP = 8
TOKENS = 49152
N_DP = 4
N_EXPERT = 128


def draw_keep_mask(key, part):
    key_list = jax.random.split(jax.random.fold_in(key, 11), EXPERTS * 2 * FW)
    orders = jax.vmap(lambda single: jax.random.permutation(single, BLOCK))(key_list)
    return (orders < KEEP).astype(jnp.int32).reshape(EXPERTS, 2, FW, BLOCK)


def draw_inv_factor(key, part):
    first, second, third = jax.random.split(jax.random.fold_in(key, 23), 3)
    diag_vec = jnp.exp(jax.random.uniform(first, (EXPERTS, BLOCK), jnp.float32, jnp.log(0.6), jnp.log(1.6)))
    spread = 0.1 * jax.random.normal(second, (EXPERTS, BLOCK, D), jnp.float32)
    rates = jax.random.uniform(third, (EXPERTS, BLOCK), jnp.float32, 0.15, 0.35)
    col_diag = jnp.concatenate([diag_vec, jnp.zeros((EXPERTS, D - BLOCK), jnp.float32)], axis=1)
    leak = rates[:, :, None] * col_diag[:, None, :]
    row_ids = jnp.arange(BLOCK)[None, :, None]
    col_ids = jnp.arange(D)[None, None, :]
    factor = jnp.where(col_ids == row_ids, diag_vec[:, :, None], jnp.where(col_ids > row_ids, leak + spread, 0.0))
    return factor.astype(jnp.float32)


def levels(key, shape, cuts, least, high):
    loudness = 1.0
    for dim, parts in cuts:
        heights = jax.random.uniform(jax.random.fold_in(jax.random.fold_in(key, 6), dim), (parts,), jnp.float32, least / len(cuts), high / len(cuts))
        loudness = loudness * jnp.repeat(jnp.exp(heights), shape[dim] // parts).reshape((-1,) + (1,) * (len(shape) - 1 - dim))
    return loudness


def deal_out(key, own, number, rows, amount, top, bound, lean):
    sequence = jax.random.permutation(key, amount)
    crowded, usual = shares(amount, rows * top, bound, lean, True), shares(amount, rows * top, bound, lean, False)
    places = jnp.arange(amount)

    def named(tallies, rotation):
        used = int((tallies > 0).sum())
        fixed = max(1, used // 4)
        shifted = fixed + (places - fixed + rotation * (used - fixed)) % max(1, amount - fixed)
        return jnp.zeros((amount,), jnp.int32).at[sequence[jnp.where(places < fixed, places, shifted)]].set(jnp.asarray(tallies, jnp.int32))

    tallies = jnp.where(number % 4 == 0, named(crowded, number // 4), named(usual, number - number // 4 - 1))
    mixed = jax.random.permutation(jax.random.fold_in(own, 3), amount)
    giver, sink = mixed[0:amount // 2 * 2:2], mixed[1:amount // 2 * 2:2]
    margin = jnp.minimum(tallies[giver] - 1, bound - tallies[sink]) // 2
    margin = jnp.where((giver == sequence[0]) | (sink == sequence[0]) | (tallies[sink] == 0), 0, jnp.maximum(margin, 0))
    shifted = jax.random.randint(jax.random.fold_in(own, 4), (amount // 2,), 0, 1 << 20) % (margin + 1)
    tallies = tallies.at[giver].add(-shifted).at[sink].add(shifted)
    items = jnp.searchsorted(jnp.cumsum(tallies), jnp.arange(rows * top), side="right").astype(jnp.int32)
    listing = items.reshape(top, rows).T
    listing = listing[jax.random.permutation(jax.random.fold_in(own, 1), rows)]
    rotation = jax.random.randint(jax.random.fold_in(own, 2), (rows, 1), 0, top)
    return jnp.take_along_axis(listing, (jnp.arange(top)[None, :] + rotation) % top, axis=1)


def shares(number_of, total, reach, skew, full):
    portions = [(1 << 20) // math.isqrt(standing ** skew) + 1 for standing in range(1, number_of + 1)]
    largest = reach if full else min(reach, max(-(-total // number_of), total * portions[0] // sum(portions)))
    least = 1 if total - largest >= number_of - 1 else 0
    holding, surplus = [largest] + [least] * (number_of - 1), total - largest - least * (number_of - 1)
    while surplus > 0:
        candidates = [i for i in range(1, number_of) if holding[i] < largest] or [i for i in range(1, number_of) if holding[i] < reach]
        whole, budget = sum([portions[i] for i in candidates]), surplus
        for i in candidates:
            addition = min(reach - holding[i], max(1, budget * portions[i] // whole), surplus)
            holding[i] = holding[i] + addition
            surplus = surplus - addition
    return np.array(holding)


def scatter_about(key, dims, deviation, limit, cuts=(), kind=jnp.bfloat16):
    drawn = deviation * jax.random.normal(key, dims, jnp.float32)
    if cuts:
        drawn = drawn * levels(key, dims, cuts, -0.22, 0.18)
    return jnp.clip(drawn, -limit, limit).astype(kind)


def setup_inputs(seed: int = 0) -> dict:
    streams_of = jax.random.split(jax.random.key(seed), 6)
    tokens = scatter_about(streams_of[0], (TOKENS, D), 1.0, 6.0, ((0, 512),))
    routes_keys = jax.random.split(jax.random.fold_in(streams_of[1], 1), TOKENS // TOK_DEV)
    routes_turns = jax.random.permutation(jax.random.fold_in(streams_of[1], 3), TOKENS // TOK_DEV)
    routes = jax.vmap(lambda own, number: deal_out(jax.random.fold_in(streams_of[1], 2), own, number, TOK_DEV, EXPERTS, TOP, CAP, 1))(routes_keys, routes_turns).reshape((TOKENS, TOP))
    weights = scatter_about(streams_of[2], (EXPERTS, 2, FW, D), D ** -0.5, 0.125, ((0, 128), (2, 4)))
    keep_mask = draw_keep_mask(jax.random.fold_in(streams_of[5], 71), 0)
    inv_factor = draw_inv_factor(jax.random.fold_in(streams_of[5], 71), 0)
    return dict(tokens=tokens, routes=routes, weights=weights, keep_mask=keep_mask, inv_factor=inv_factor)


def prune_rows(weights, keep_mask, inv_factor):
    block_width = keep_mask.shape[-1]
    initial = weights.astype(jnp.float32)
    leading = initial[..., :block_width]
    dropped = (1 - keep_mask).astype(jnp.float32)
    factor_block = inv_factor[:, :, :block_width]

    def column(column_id, state):
        leading, errors = state
        current = lax.dynamic_index_in_dim(leading, column_id, 3, keepdims=False)
        factor_row = lax.dynamic_index_in_dim(factor_block, column_id, 1, keepdims=False)
        diagonal = lax.dynamic_index_in_dim(factor_row, column_id, 1, keepdims=False)
        error_col = lax.dynamic_index_in_dim(dropped, column_id, 3, keepdims=False) * current / diagonal[:, None, None]
        leading = leading - error_col[..., None] * factor_row[:, None, None, :]
        errors = lax.dynamic_update_index_in_dim(errors, error_col, column_id, 3)
        return leading, errors

    leading, errors = lax.fori_loop(0, block_width, column, (leading, jnp.zeros_like(leading)))
    trailing = initial[..., block_width:] - jnp.einsum("epri,eij->eprj", errors, inv_factor[:, :, block_width:], precision=lax.Precision.HIGHEST)
    return jnp.concatenate([leading, trailing], axis=-1).astype(jnp.bfloat16)


def reference(tokens, routes, weights, keep_mask, inv_factor):
    def prune_one(packed):
        return prune_rows(packed[0][None], packed[1][None], packed[2][None])[0]

    pruned = lax.map(prune_one, (weights, keep_mask, inv_factor))
    slot_expert = routes.reshape(-1).astype(jnp.int32)
    slot_total = slot_expert.shape[0]
    by_expert = jnp.argsort(slot_expert, stable=True).astype(jnp.int32)
    per_expert = jnp.bincount(slot_expert, length=EXPERTS).astype(jnp.int32)
    expert_start = (jnp.cumsum(per_expert) - per_expert).astype(jnp.int32)
    group_rows = CAP * N_DP * N_EXPERT
    padded_order = jnp.concatenate([by_expert, jnp.full((group_rows,), slot_total, jnp.int32)])

    def expert_step(hidden_all, expert_id):
        slot_ids = lax.dynamic_slice_in_dim(padded_order, expert_start[expert_id], group_rows)
        is_live = jnp.arange(group_rows, dtype=jnp.int32) < per_expert[expert_id]
        slot_ids = jnp.where(is_live, slot_ids, slot_total).astype(jnp.int32)
        chosen = tokens[jnp.minimum(slot_ids, slot_total - 1) // TOP].astype(jnp.float32)
        gate_out = jnp.dot(chosen, pruned[expert_id, 0].astype(jnp.float32).T, preferred_element_type=jnp.float32)
        up_out = jnp.dot(chosen, pruned[expert_id, 1].astype(jnp.float32).T, preferred_element_type=jnp.float32)
        hidden_rows = (jax.nn.silu(gate_out) * up_out).astype(jnp.bfloat16)
        hidden_all = hidden_all.at[slot_ids].set(hidden_rows, mode="drop")
        return hidden_all, None

    hidden_all = jnp.zeros((slot_total, FW), jnp.bfloat16)
    hidden_all, _ = lax.scan(expert_step, hidden_all, jnp.arange(EXPERTS, dtype=jnp.int32))
    return hidden_all.reshape(TOKENS, TOP, FW)
```

```python
import functools

import jax
import jax.numpy as jnp
from jax import lax
from jax.experimental import pallas as pl
from jax.experimental.pallas import tpu as pltpu
from jax.sharding import PartitionSpec as P

MESH = pl.DeviceIdType.MESH
F32 = jnp.float32
BF16 = jnp.bfloat16
HI = lax.Precision.HIGHEST
BLK = 128
SUB = 16
SLOTS = 8
TILE = 256
NY, NZ, NC = 4, 16, 2


def iota(shape, dim):
    return lax.broadcasted_iota(jnp.int32, shape, dim)


def dot(a, b, dims, precision=None):
    return lax.dot_general(
        a, b, (dims, ((), ())), precision=precision, preferred_element_type=F32
    )

def prune_body(w_ref, mask_ref, f_ref, out_ref):
    factor = f_ref[:, :BLK]
    row_id = lax.broadcasted_iota(jnp.int32, (BLK, BLK), 0)
    col_id = lax.broadcasted_iota(jnp.int32, (BLK, BLK), 1)
    diagonal = jnp.sum(jnp.where(row_id == col_id, factor, 0.0), axis=1, keepdims=True)
    factor_t = factor.T
    lead = w_ref[:, :BLK].astype(F32).T
    scale = (1 - mask_ref[...]).astype(F32).T / diagonal
    errors, done = [], []
    for start in range(0, BLK, SUB):
        part = lead[:SUB]
        rows = []
        for i in range(SUB):
            g = start + i
            err = part[i : i + 1] * scale[g : g + 1]
            part = part - factor_t[start : start + SUB, g : g + 1] * err
            rows.append(err)
        block = jnp.concatenate(rows, axis=0)
        errors.append(block)
        done.append(part)
        if start + SUB < BLK:
            upd = lax.dot_general(
                factor[start : start + SUB], block, (((0,), (0,)), ((), ())),
                precision=HI, preferred_element_type=F32,
            )
            lead = lead[SUB:] - upd[start + SUB :]
    err_all = jnp.concatenate(errors, axis=0).T
    out_ref[:, :BLK] = jnp.concatenate(done, axis=0).T.astype(out_ref.dtype)
    step = 384
    for at in range(BLK, w_ref.shape[1], step):
        upd = lax.dot_general(
            err_all, f_ref[:, at : at + step], (((1,), (0,)), ((), ())),
            precision=HI, preferred_element_type=F32,
        )
        out_ref[:, at : at + step] = (w_ref[:, at : at + step].astype(F32) - upd).astype(out_ref.dtype)


def prune(weights, keep_mask, inv_factor):
    p, r, d = weights.shape[1:]
    return pl.pallas_call(
        prune_body,
        out_shape=jax.ShapeDtypeStruct((p * r, d), jnp.bfloat16),
        in_specs=[pl.BlockSpec(memory_space=pltpu.VMEM)] * 3,
        out_specs=pl.BlockSpec(memory_space=pltpu.VMEM),
        name="prune",
    )(weights.reshape(p * r, d), keep_mask.reshape(p * r, BLK), inv_factor.reshape(BLK, d))


def exchange_body(nx, tok, routes, pruned, out, t_up, t_down, rt_own, rt, packed, rows, whole, batch_rows,
                  hid, back, home, code, bar_sems, ring_s, ring_r, rt_s, rt_r, x_s, x_r, own_s,
                  ys_s, ys_r, zs_s, zs_r, hs_s, hs_r, loc_s):
    del bar_sems
    tokens, width = tok.shape
    top = routes.shape[1]
    slots_all = tokens * top
    own_rows = pruned.shape[0] // 2
    half = NZ // 2
    peers = NY * NC
    batch = min(4, NZ)
    batches = NZ // batch
    x = lax.axis_index("dp")
    me = lax.axis_index("expert")
    y = me // (NZ * NC)
    z = (me // NC) % NZ
    c = me % NC

    def along_z(n):
        return {"expert": (y * NZ + (z + n) % NZ) * NC + c}

    def along_y(q):
        return {"expert": (((y + q // NC) % NY) * NZ + z) * NC + (c + q % NC) % NC}

    def along_x(n):
        return {"dp": (x + n) % nx}

    def mirror(q):
        return ((NY - q // NC) % NY) * NC + q % NC

    def remote(src, dst, s, r, device):
        return pltpu.make_async_remote_copy(
            src_ref=src, dst_ref=dst, send_sem=s, recv_sem=r, device_id=device, device_id_type=MESH
        )

    barrier = pltpu.get_barrier_semaphore()
    met = [along_z(n) for n in range(1, NZ)] + [along_y(q) for q in range(1, peers)]
    if nx > 1:
        met += [along_x(1), along_x(nx - 1)]
    for device in met:
        pl.semaphore_signal(barrier, inc=1, device_id=device, device_id_type=MESH)
    pl.semaphore_wait(barrier, len(met))

    part = tokens // 2

    def ring(way, s, h):
        span = pl.ds(h * part, part)
        held = t_up if way == 0 or s == half else t_down
        before = t_up if way == 0 else t_down
        src = tok.at[span] if s == 1 else before.at[s - 1, span]
        at = (s * 2 + way) * 2 + h
        return remote(src, held.at[s, span], ring_s.at[at], ring_r.at[at], along_z(1 if way == 0 else NZ - 1))

    def ring_has(way, s, h):
        return s < half or (s == half and h == way)

    for h in range(2):
        for way in range(2):
            if ring_has(way, 1, h):
                ring(way, 1, h).start()

    x_copies, x_forward = [], []
    span_own = [pl.ds(g * own_rows, own_rows) for g in range(2)]

    def place(g, n):
        return whole.at[g, pl.ds(pl.multiple_of(((x + n) % nx) * own_rows, own_rows), own_rows)]

    own_copies = [pltpu.make_async_copy(pruned.at[span_own[g]], place(g, 0), own_s.at[g]) for g in range(2)]
    for copy in own_copies:
        copy.start()
    if nx > 1:
        for i, (n, g) in enumerate(((1, 0), (nx - 1, 1), (1, 1), (nx - 1, 0))):
            copy = remote(pruned.at[span_own[g]], place(g, 0), x_s.at[i], x_r.at[i], along_x(n))
            copy.start()
            x_copies.append(copy)

    chosen = routes[...].astype(F32).astype(BF16)
    eye = (iota((tokens, BLK), 0) == iota((tokens, BLK), 1)).astype(F32).astype(BF16)
    turned = dot(chosen, eye, ((0,), (0,)))
    turned = jnp.where(iota((top, BLK), 1) < tokens, turned, -1.0)
    rt_own[...] = turned
    rt[0] = turned

    repeat = (iota((slots_all, tokens), 0) // top == iota((slots_all, tokens), 1)).astype(F32).astype(BF16)
    spread = dot(repeat, chosen, ((1,), (0,)))
    mine = iota((slots_all, top), 0) % top == iota((slots_all, top), 1)
    expert_of = jnp.sum(jnp.where(mine, spread, 0.0), axis=1, keepdims=True)
    hot = (expert_of == iota((slots_all, NY * NZ * NC), 1).astype(F32)).astype(F32)
    earlier = (iota((slots_all, slots_all), 1) < iota((slots_all, slots_all), 0)).astype(F32).astype(BF16)
    ranks = dot(earlier, hot.astype(BF16), ((1,), (0,)))
    each = iota((1, NY * NZ * NC), 1)
    rel = (each // NC % NZ - z + NZ) % NZ
    pos = jnp.where(rel < half, 2 * (half - rel), 2 * (rel - half) + 1)
    pos = jnp.where(rel == half, 0, jnp.where(rel == 0, 1, pos))
    peer = (each // (NZ * NC) - y + NY) % NY * NC + (each % NC - c + NC) % NC
    table = ((pos * peers + peer) * SLOTS).astype(F32)
    code[...] = jnp.broadcast_to(jnp.sum(hot * (ranks + table), axis=1, keepdims=True), code.shape)

    if NZ > 1:
        for n in range(1, NZ):
            remote(rt_own, rt.at[(NZ - n) % NZ], rt_s, rt_r, along_z(n)).start()
        pltpu.make_async_copy(rt.at[pl.ds(1, NZ - 1)], rt.at[pl.ds(1, NZ - 1)], rt_r).wait()

    q_id = iota((peers, BLK), 0)
    experts = (((y + q_id // NC) % NY * NZ + z) * NC + (c + q_id % NC) % NC).astype(F32)
    before_token = (iota((BLK, BLK), 0) < iota((BLK, BLK), 1)).astype(F32).astype(BF16)

    def pack(position, n, block):
        named = rt[n]
        hit = jnp.zeros((peers, BLK), F32)
        for k in range(top):
            hit = hit + (named[k : k + 1] == experts).astype(F32)
        rank = dot(hit.astype(BF16), before_token, ((1,), (0,)))
        key = jnp.where(hit > 0, rank, -1.0)
        pick = (key[:, None, :] == iota((peers, SLOTS, BLK), 1).astype(F32)).astype(F32)
        pick = pick.reshape(peers * SLOTS, BLK).astype(BF16)[:, :tokens]
        for at in range(0, width, min(512, width)):
            cols = pl.ds(at, min(512, width))
            taken = dot(pick, block[:, cols], ((1,), (0,)))
            taken = taken.reshape(peers, SLOTS, min(512, width)).astype(BF16)
            packed[position, :, :, cols] = taken
            rows[position, 0, :, cols] = taken[0]

    def to_peer(position, q):
        return remote(packed.at[position, q], rows.at[position, mirror(q)], ys_s.at[position], ys_r.at[position], along_y(q))

    def hand_out(position):
        for q in range(1, peers):
            to_peer(position, q).start()

    pack(1, 0, tok)
    hand_out(1)
    for s in range(1, half + 1):
        for h in range(2):
            for way in range(2):
                if ring_has(way, s, h):
                    ring(way, s, h).wait_recv()
                    if ring_has(way, s + 1, h):
                        ring(way, s + 1, h).start()
        if nx > 1 and s == min(3, half):
            x_copies[0].wait_recv()
            x_copies[1].wait_recv()
            for i, (g, n) in enumerate(((0, 1), (1, nx - 1))):
                copy = remote(place(g, nx - n), place(g, nx - n), x_s.at[4 + i], x_r.at[4 + i], along_x(n))
                copy.start()
                x_forward.append(copy)
        if s < half:
            pack(2 * (half - s), s, t_down.at[s])
            pack(2 * (half - s) + 1, NZ - s, t_up.at[s])
            hand_out(2 * (half - s))
            hand_out(2 * (half - s) + 1)
        else:
            pack(0, half, t_up.at[half])
            hand_out(0)

    for copy in own_copies:
        copy.wait()
    for copy in x_copies[2:] + x_forward:
        copy.wait_recv()

    def to_line(m, later):
        p = 2 * m + later
        n = half + m if later else half - m
        return remote(hid.at[p], back.at[2 * m + 1 - later], zs_s.at[p], zs_r.at[2 * m + 1 - later], along_z(n))

    far = remote(hid.at[0], back.at[0], zs_s.at[0], zs_r.at[0], along_z(half))
    here = pltpu.make_async_copy(hid.at[1], back.at[1], zs_r.at[1])

    def work(b, carry):
        first = b * batch
        for k in range(batch):
            if peers > 1:
                landed = rows.at[first + k, pl.ds(1, peers - 1)]
                pltpu.make_async_copy(landed, landed, ys_r.at[first + k]).wait()
        count = batch * peers * SLOTS
        batch_rows[...] = rows[pl.ds(first, batch)].astype(F32).reshape(count, width).astype(BF16)
        for at in range(0, whole.shape[1], TILE):
            cols = pl.ds(at, TILE)
            gate = dot(batch_rows[...], whole[0, cols], ((1,), (1,)))
            up = dot(batch_rows[...], whole[1, cols], ((1,), (1,)))
            value = gate / (1.0 + jnp.exp(-gate)) * up
            hid[pl.ds(first, batch), :, :, cols] = value.reshape(batch, peers, SLOTS, TILE).astype(BF16)

        @pl.when(b == 0)
        def _():
            far.start()
            here.start()

        @pl.when(b > 0)
        def _():
            to_line(b * (batch // 2), 0).start()
            to_line(b * (batch // 2), 1).start()

        for j in range(1, batch // 2):
            to_line(b * (batch // 2) + j, 0).start()
            to_line(b * (batch // 2) + j, 1).start()
        return carry

    lax.fori_loop(0, batches, work, 0)

    def homeward(b, q):
        span = pl.ds(b * batch, batch)
        return remote(back.at[span, q], home.at[span, mirror(q)], hs_s.at[b], hs_r.at[b], along_y(q))

    def stay(b):
        span = pl.ds(b * batch, batch)
        return pltpu.make_async_copy(back.at[span, 0], home.at[span, 0], loc_s.at[b])

    out[...] = jnp.zeros(out.shape, out.dtype)

    def finish(b, carry):
        @pl.when(b < batches)
        def _():
            for k in range(batch):
                block = back.at[b * batch + k]
                pltpu.make_async_copy(block, block, zs_r.at[b * batch + k]).wait()
            stay(b).start()
            for q in range(1, peers):
                homeward(b, q).start()

        @pl.when(b > 0)
        def _():
            last = b - 1
            span = pl.ds(last * batch, batch)
            stay(last).wait()
            if peers > 1:
                landed = home.at[span, pl.ds(1, peers - 1)]
                pltpu.make_async_copy(landed, landed, hs_r.at[last]).wait()
            count = batch * peers * SLOTS
            values = home[span].astype(F32).reshape(count, out.shape[1]).astype(BF16)
            wanted = (iota((slots_all, BLK), 1) + last * count).astype(F32)
            pick = [(code[...] == wanted + float(at)).astype(F32).astype(BF16) for at in range(0, count, BLK)]
            pick = jnp.concatenate(pick, axis=1)[:, :count]
            for at in range(0, out.shape[1], TILE):
                cols = pl.ds(at, TILE)
                got = dot(pick, values[:, at : at + TILE], ((1,), (0,)))
                out[:, cols] = (out[:, cols].astype(F32) + got).astype(BF16)
        return carry

    lax.fori_loop(0, batches + 1, finish, 0)

    for s in range(1, half + 1):
        for h in range(2):
            for way in range(2):
                if ring_has(way, s, h):
                    ring(way, s, h).wait_send()
    for copy in x_copies + x_forward:
        copy.wait_send()
    if NZ > 1:
        pltpu.make_async_copy(rt.at[pl.ds(1, NZ - 1)], rt.at[pl.ds(1, NZ - 1)], rt_s).wait()

    def drain(p, carry):
        if peers > 1:
            pltpu.make_async_copy(packed.at[p, pl.ds(1, peers - 1)], packed.at[p, pl.ds(1, peers - 1)], ys_s.at[p]).wait()

        @pl.when(p != 1)
        def _():
            pltpu.make_async_copy(hid.at[p], hid.at[p], zs_s.at[p]).wait()
        return carry

    lax.fori_loop(0, NZ, drain, 0)

    def drain_home(b, carry):
        if peers > 1:
            sent = back.at[pl.ds(b * batch, batch), pl.ds(1, peers - 1)]
            pltpu.make_async_copy(sent, sent, hs_s.at[b]).wait()
        return carry

    lax.fori_loop(0, batches, drain_home, 0)


def exchange(tokens, routes, pruned):
    nx = lax.axis_size("dp")
    count, width = tokens.shape
    top = routes.shape[1]
    hidden = pruned.shape[0] // 2 * nx
    half, peers = NZ // 2, NY * NC
    batch = min(4, NZ)
    dma = pltpu.SemaphoreType.DMA
    out = pl.pallas_call(
        functools.partial(exchange_body, nx),
        out_shape=jax.ShapeDtypeStruct((count * top, hidden), BF16),
        in_specs=[pl.BlockSpec(memory_space=pltpu.VMEM)] * 3,
        out_specs=pl.BlockSpec(memory_space=pltpu.VMEM),
        scratch_shapes=[
            pltpu.VMEM((half + 1, count, width), BF16),
            pltpu.VMEM((half, count, width), BF16),
            pltpu.VMEM((top, BLK), F32),
            pltpu.VMEM((NZ, top, BLK), F32),
            pltpu.VMEM((NZ, peers, SLOTS, width), BF16),
            pltpu.VMEM((NZ, peers, SLOTS, width), BF16),
            pltpu.VMEM((2, hidden, width), BF16),
            pltpu.VMEM((batch * peers * SLOTS, width), BF16),
            pltpu.VMEM((NZ, peers, SLOTS, hidden), BF16),
            pltpu.VMEM((NZ, peers, SLOTS, hidden), BF16),
            pltpu.VMEM((NZ, peers, SLOTS, hidden), BF16),
            pltpu.VMEM((count * top, BLK), F32),
            dma((1,)),
            dma(((half + 1) * 4,)),
            dma(((half + 1) * 4,)),
            dma(()),
            dma(()),
            dma((6,)),
            dma((6,)),
            dma((2,)),
            dma((NZ,)),
            dma((NZ,)),
            dma((NZ,)),
            dma((NZ,)),
            dma((NZ // batch,)),
            dma((NZ // batch,)),
            dma((NZ // batch,)),
        ],
        compiler_params=pltpu.CompilerParams(
            collective_id=0, has_side_effects=True, vmem_limit_bytes=60 * 1024 * 1024
        ),
        name="exchange",
    )(tokens, routes, pruned)
    return out.reshape(count, top, hidden)


def local(tokens, routes, weights, keep_mask, inv_factor):
    pruned = prune(weights, keep_mask, inv_factor)
    return exchange(tokens, routes, pruned)


def solution(mesh):
    return jax.shard_map(
        local,
        mesh=mesh,
        in_specs=(
            P(("dp", "expert"), None),
            P(("dp", "expert"), None),
            P("expert", None, "dp", None),
            P("expert", None, "dp", None),
            P("expert", None, None),
        ),
        out_specs=P(("dp", "expert"), None, None),
        check_vma=False,
    )
```

```python
import functools

import jax
import jax.numpy as jnp
from jax import lax
from jax.experimental import pallas as pl
from jax.experimental.pallas import tpu as pltpu
from jax.sharding import PartitionSpec as P

MESH = pl.DeviceIdType.MESH
F32 = jnp.float32
BF16 = jnp.bfloat16
HI = lax.Precision.HIGHEST
BLK = 128
SUB = 16
SLOTS = 8
TILE = 256
CHUNKS = 3
X_STEP = 3
VMEM_MIB = 60
FAR_MET = ()
NY, NZ, NC = 4, 16, 2
ORDER = (4, 5, 3, 6, 7, 8, 1, 2)
EARLY = {7: (0,)}


def iota(shape, dim):
    return lax.broadcasted_iota(jnp.int32, shape, dim)


def dot(a, b, dims, precision=None):
    return lax.dot_general(
        a, b, (dims, ((), ())), precision=precision, preferred_element_type=F32
    )


def prune_body(w_ref, mask_ref, f_ref, out_ref):
    factor = f_ref[:, :BLK]
    row_id = lax.broadcasted_iota(jnp.int32, (BLK, BLK), 0)
    col_id = lax.broadcasted_iota(jnp.int32, (BLK, BLK), 1)
    diagonal = jnp.sum(jnp.where(row_id == col_id, factor, 0.0), axis=1, keepdims=True)
    factor_t = factor.T
    lead = w_ref[:, :BLK].astype(F32).T
    scale = (1 - mask_ref[...]).astype(F32).T / diagonal
    errors, done = [], []
    for start in range(0, BLK, SUB):
        part = lead[:SUB]
        rows = []
        for i in range(SUB):
            g = start + i
            err = part[i : i + 1] * scale[g : g + 1]
            part = part - factor_t[start : start + SUB, g : g + 1] * err
            rows.append(err)
        block = jnp.concatenate(rows, axis=0)
        errors.append(block)
        done.append(part)
        if start + SUB < BLK:
            upd = lax.dot_general(
                factor[start : start + SUB], block, (((0,), (0,)), ((), ())),
                precision=HI, preferred_element_type=F32,
            )
            lead = lead[SUB:] - upd[start + SUB :]
    err_all = jnp.concatenate(errors, axis=0).T
    out_ref[:, :BLK] = jnp.concatenate(done, axis=0).T.astype(out_ref.dtype)
    step = 384
    for at in range(BLK, w_ref.shape[1], step):
        upd = lax.dot_general(
            err_all, f_ref[:, at : at + step], (((1,), (0,)), ((), ())),
            precision=HI, preferred_element_type=F32,
        )
        out_ref[:, at : at + step] = (w_ref[:, at : at + step].astype(F32) - upd).astype(out_ref.dtype)


def exchange_body(nx, tok_in, routes_in, weights_in, mask_in, factor_in, out, tok, weights, mask, factor, pruned,
                  t_up, t_down, rt, packed, rows, whole, batch_rows, hid, back, home, code, load_s, ring_s, ring_r,
                  rt_s, rt_r, x_s, x_r, own_s, ys_s, ys_r, zs_s, zs_r, hs_s, hs_r, loc_s):
    tokens, width = tok.shape
    top = routes_in.shape[0]
    slots_all = tokens * top
    own_rows = pruned.shape[0] // 2
    half = NZ // 2
    peers = NY * NC
    owners = NY * NZ * NC
    order = [n for s in ORDER for n in ((s, NZ - s) if s < half else (half, 0))]
    pos_of = {n: p for p, n in enumerate(order)}
    batch = min(4, NZ)
    batches = NZ // batch
    x = lax.axis_index("dp")
    me = lax.axis_index("expert")
    y = me // (NZ * NC)
    z = (me // NC) % NZ
    c = me % NC

    loads = [
        pltpu.make_async_copy(src, dst, load_s.at[i])
        for i, (src, dst) in enumerate(((tok_in, tok), (weights_in, weights), (mask_in, mask), (factor_in, factor)))
    ]
    for copy in loads:
        copy.start()

    def along_z(n):
        return {"expert": (y * NZ + (z + n) % NZ) * NC + c}

    def along_y(q):
        return {"expert": (((y + q // NC) % NY) * NZ + z) * NC + (c + q % NC) % NC}

    def along_x(n):
        return {"dp": (x + n) % nx}

    def mirror(q):
        return ((NY - q // NC) % NY) * NC + q % NC

    def remote(src, dst, s, r, device):
        return pltpu.make_async_remote_copy(
            src_ref=src, dst_ref=dst, send_sem=s, recv_sem=r, device_id=device, device_id_type=MESH
        )

    barrier = pltpu.get_barrier_semaphore()
    met = [along_z(n) for n in (FAR_MET if FAR_MET else sorted({1, NZ - 1}))] + [along_y(q) for q in range(1, peers)]
    if nx > 1:
        met += [along_x(1), along_x(nx - 1)]
    for device in met:
        pl.semaphore_signal(barrier, inc=1, device_id=device, device_id_type=MESH)
    pl.semaphore_wait(barrier, len(met))

    chunk = tokens // CHUNKS

    def ring_rows(way, s, h):
        low, high = h * chunk, h * chunk + chunk
        if s == half:
            low, high = (low, min(high, tokens // 2)) if way == 0 else (max(low, tokens // 2), high)
        return low, high

    def ring_has(way, s, h):
        low, high = ring_rows(way, s, h)
        return s <= half and low < high

    def ring(way, s, h):
        low, high = ring_rows(way, s, h)
        span = pl.ds(low, high - low)
        held = t_up if way == 0 or s == half else t_down
        src = tok.at[span] if s == 1 else (t_up if way == 0 else t_down).at[s - 1, span]
        at = ((s - 1) * 2 + way) * CHUNKS + h
        return remote(src, held.at[s, span], ring_s.at[at], ring_r.at[at], along_z(1 if way == 0 else NZ - 1))

    def names(way, s):
        at = (s - 1) * 2 + way
        src, dst = (NZ - s + 1) % NZ if way == 0 else s - 1, NZ - s if way == 0 else s
        return remote(rt.at[src], rt.at[dst], rt_s.at[at], rt_r.at[at], along_z(1 if way == 0 else NZ - 1))

    def names_has(way, s):
        return s < half or (s == half and way == 0)

    loads[0].wait()
    for h in range(CHUNKS):
        for way in range(2):
            if ring_has(way, 1, h):
                ring(way, 1, h).start()

    rt[0] = jnp.full((top, BLK), -1.0, F32)
    rt[0, :, pl.ds(0, tokens)] = routes_in[...].astype(F32)

    for copy in loads[1:]:
        copy.wait()
    prune_body(weights, mask, factor, pruned)

    x_copies, x_forward = [], []
    span_own = [pl.ds(g * own_rows, own_rows) for g in range(2)]

    def place(g, n):
        return whole.at[g, pl.ds(pl.multiple_of(((x + n) % nx) * own_rows, own_rows), own_rows)]

    for way in range(2):
        if names_has(way, 1):
            names(way, 1).start()
    own_copies = [pltpu.make_async_copy(pruned.at[span_own[g]], place(g, 0), own_s.at[g]) for g in range(2)]
    if nx > 1:
        for i, (n, g) in enumerate(((1, 0), (nx - 1, 1), (1, 1), (nx - 1, 0))):
            copy = remote(pruned.at[span_own[g]], place(g, 0), x_s.at[i], x_r.at[i], along_x(n))
            copy.start()
            x_copies.append(copy)
    for copy in own_copies:
        copy.start()

    def forward_weights():
        if nx > 1:
            x_copies[0].wait_recv()
            x_copies[1].wait_recv()
            for i, (g, n) in enumerate(((0, 1), (1, nx - 1))):
                copy = remote(place(g, nx - n), place(g, nx - n), x_s.at[4 + i], x_r.at[4 + i], along_x(n))
                copy.start()
                x_forward.append(copy)

    def find_code():
        lane = (iota((tokens, BLK), 0) == iota((tokens, BLK), 1)).astype(F32).astype(BF16)
        chosen = dot(lane, rt[0].astype(BF16), ((1,), (1,))).astype(BF16)
        repeat = (iota((slots_all, tokens), 0) // top == iota((slots_all, tokens), 1)).astype(F32).astype(BF16)
        spread = dot(repeat, chosen, ((1,), (0,)))
        mine = iota((slots_all, top), 0) % top == iota((slots_all, top), 1)
        expert_of = jnp.sum(jnp.where(mine, spread, 0.0), axis=1, keepdims=True)
        hot = (expert_of == iota((slots_all, owners), 1).astype(F32)).astype(F32)
        earlier = (iota((slots_all, slots_all), 1) < iota((slots_all, slots_all), 0)).astype(F32).astype(BF16)
        ranks = dot(earlier, hot.astype(BF16), ((1,), (0,)))
        each = iota((1, owners), 1)
        rel = (each // NC % NZ - z + NZ) % NZ
        pos = jnp.zeros_like(rel)
        for n, p in pos_of.items():
            pos = jnp.where(rel == n, p, pos)
        peer = (each // (NZ * NC) - y + NY) % NY * NC + (each % NC - c + NC) % NC
        table = ((pos * peers + peer) * SLOTS).astype(F32)
        code[...] = jnp.broadcast_to(jnp.sum(hot * (ranks + table), axis=1, keepdims=True), code.shape)

    q_id = iota((peers, BLK), 0)
    experts = (((y + q_id // NC) % NY * NZ + z) * NC + (c + q_id % NC) % NC).astype(F32)
    before_token = (iota((BLK, BLK), 0) < iota((BLK, BLK), 1)).astype(F32).astype(BF16)

    def pack(n, block):
        position = pos_of[n]
        named = rt[n]
        hit = jnp.zeros((peers, BLK), F32)
        for k in range(top):
            hit = hit + (named[k : k + 1] == experts).astype(F32)
        rank = dot(hit.astype(BF16), before_token, ((1,), (0,)))
        key = jnp.where(hit > 0, rank, -1.0)
        pick = (key[:, None, :] == iota((peers, SLOTS, BLK), 1).astype(F32)).astype(F32)
        pick = pick.reshape(peers * SLOTS, BLK).astype(BF16)[:, :tokens]
        wide = min(512, width)
        for at in range(0, width, wide):
            cols = pl.ds(at, wide)
            taken = dot(pick, block[:, cols], ((1,), (0,)))
            taken = taken.reshape(peers, SLOTS, wide).astype(BF16)
            packed[position, :, :, cols] = taken
            rows[position, 0, :, cols] = taken[0]

    def to_peer(position, q):
        return remote(packed.at[position, q], rows.at[position, mirror(q)], ys_s.at[position], ys_r.at[position], along_y(q))

    packed_last = []

    def pack_next(n, block):
        pack(n, block)
        hand_out()
        packed_last.append(pos_of[n])

    def hand_out():
        while packed_last:
            position = packed_last.pop()
            for q in range(1, peers):
                to_peer(position, q).start()

    def return_to(n):
        p, q = pos_of[n], pos_of[(NZ - n) % NZ]
        if n == 0:
            return pltpu.make_async_copy(hid.at[p], back.at[p], zs_r.at[p])
        return remote(hid.at[p], back.at[q], zs_s.at[p], zs_r.at[q], along_z(n))

    def work(b):
        first = b * batch
        if peers > 1:
            for k in range(batch):
                landed = rows.at[first + k, pl.ds(1, peers - 1)]
                pltpu.make_async_copy(landed, landed, ys_r.at[first + k]).wait()
        count = batch * peers * SLOTS
        batch_rows[...] = rows[pl.ds(first, batch)].astype(F32).reshape(count, width).astype(BF16)
        for at in range(0, whole.shape[1], TILE):
            cols = pl.ds(at, TILE)
            gate = dot(batch_rows[...], whole[0, cols], ((1,), (1,)))
            up = dot(batch_rows[...], whole[1, cols], ((1,), (1,)))
            value = gate / (1.0 + jnp.exp(-gate)) * up
            hid[pl.ds(first, batch), :, :, cols] = value.reshape(batch, peers, SLOTS, TILE).astype(BF16)
        for n in sorted(order[first : first + batch], key=lambda n: -min(n, NZ - n)):
            return_to(n).start()

    def have_weights():
        for copy in own_copies:
            copy.wait()
        for copy in x_copies[2:] + x_forward:
            copy.wait_recv()

    jobs = {(1, 0): [lambda: pack_next(0, tok)], (1, 1): [find_code]}
    for s in range(1, half):
        jobs.setdefault((s + 1, 0), []).append(lambda s=s: pack_next(NZ - s, t_up.at[s]))
        jobs.setdefault((s + 1, 1), []).append(lambda s=s: pack_next(s, t_down.at[s]))
    jobs.setdefault((min(X_STEP, half), 2), []).append(forward_weights)
    for s, early in EARLY.items():
        jobs.setdefault((s, CHUNKS - 1), []).append(have_weights)
        for b in early:
            jobs[s, CHUNKS - 1].append(lambda b=b: work(b))
    for s in range(1, half + 1):
        for h in range(CHUNKS):
            for way in range(2):
                if h == 0 and names_has(way, s):
                    names(way, s).wait_recv()
                    if names_has(way, s + 1):
                        names(way, s + 1).start()
                if ring_has(way, s, h):
                    ring(way, s, h).wait_recv()
                    if ring_has(way, s + 1, h):
                        ring(way, s + 1, h).start()
            for job in jobs.get((s, h), []):
                job()
    pack_next(half, t_up.at[half])
    hand_out()
    if not EARLY:
        have_weights()
    for b in range(batches):
        if not any(b in early for early in EARLY.values()):
            work(b)

    def homeward(b, q):
        span = pl.ds(b * batch, batch)
        return remote(back.at[span, q], home.at[span, mirror(q)], hs_s.at[b], hs_r.at[b], along_y(q))

    def stay(b):
        span = pl.ds(b * batch, batch)
        return pltpu.make_async_copy(back.at[span, 0], home.at[span, 0], loc_s.at[b])

    def send_home(b):
        for k in range(batch):
            block = back.at[b * batch + k]
            pltpu.make_async_copy(block, block, zs_r.at[b * batch + k]).wait()
        stay(b).start()
        for q in range(1, peers):
            homeward(b, q).start()

    def unpack(b):
        span = pl.ds(b * batch, batch)
        stay(b).wait()
        if peers > 1:
            landed = home.at[span, pl.ds(1, peers - 1)]
            pltpu.make_async_copy(landed, landed, hs_r.at[b]).wait()
        count = batch * peers * SLOTS
        values = home[span].astype(F32).reshape(count, out.shape[1]).astype(BF16)
        lanes = iota((slots_all, BLK), 1).astype(F32)
        pick = [(code[...] == lanes + float(b * count + at)).astype(F32).astype(BF16) for at in range(0, count, BLK)]
        pick = jnp.concatenate(pick, axis=1)[:, :count]
        for at in range(0, out.shape[1], TILE):
            cols = pl.ds(at, TILE)
            got = dot(pick, values[:, at : at + TILE], ((1,), (0,)))
            if b > 0:
                got = out[:, cols].astype(F32) + got
            out[:, cols] = got.astype(BF16)

    for b in range(batches):
        send_home(b)
        if b > 0:
            unpack(b - 1)
    unpack(batches - 1)

    for s in range(1, half + 1):
        for way in range(2):
            if names_has(way, s):
                names(way, s).wait_send()
            for h in range(CHUNKS):
                if ring_has(way, s, h):
                    ring(way, s, h).wait_send()
    for copy in x_copies + x_forward:
        copy.wait_send()
    for p in range(NZ):
        if peers > 1:
            sent = packed.at[p, pl.ds(1, peers - 1)]
            pltpu.make_async_copy(sent, sent, ys_s.at[p]).wait()
        if order[p] != 0:
            pltpu.make_async_copy(hid.at[p], hid.at[p], zs_s.at[p]).wait()
    if peers > 1:
        for b in range(batches):
            sent = back.at[pl.ds(b * batch, batch), pl.ds(1, peers - 1)]
            pltpu.make_async_copy(sent, sent, hs_s.at[b]).wait()


def exchange(tokens, routes, weights, keep_mask, factor):
    nx = lax.axis_size("dp")
    count, width = tokens.shape
    top = routes.shape[1]
    own = weights.shape[0]
    hidden = own // 2 * nx
    half, peers = NZ // 2, NY * NC
    batch = min(4, NZ)
    dma = pltpu.SemaphoreType.DMA
    vmem = pltpu.VMEM
    out = pl.pallas_call(
        functools.partial(exchange_body, nx),
        out_shape=jax.ShapeDtypeStruct((count * top, hidden), BF16),
        in_specs=[
            pl.BlockSpec(memory_space=pltpu.HBM),
            pl.BlockSpec(memory_space=pltpu.VMEM),
            pl.BlockSpec(memory_space=pltpu.HBM),
            pl.BlockSpec(memory_space=pltpu.HBM),
            pl.BlockSpec(memory_space=pltpu.HBM),
        ],
        out_specs=pl.BlockSpec(memory_space=pltpu.VMEM),
        scratch_shapes=[
            vmem((count, width), BF16),
            vmem((own, width), BF16),
            vmem((own, BLK), jnp.int32),
            vmem((BLK, width), F32),
            vmem((own, width), BF16),
            vmem((half + 1, count, width), BF16),
            vmem((half, count, width), BF16),
            vmem((NZ, top, BLK), F32),
            vmem((NZ, peers, SLOTS, width), BF16),
            vmem((NZ, peers, SLOTS, width), BF16),
            vmem((2, hidden, width), BF16),
            vmem((batch * peers * SLOTS, width), BF16),
            vmem((NZ, peers, SLOTS, hidden), BF16),
            vmem((NZ, peers, SLOTS, hidden), BF16),
            vmem((NZ, peers, SLOTS, hidden), BF16),
            vmem((count * top, BLK), F32),
            dma((4,)),
            dma((half * 2 * CHUNKS,)),
            dma((half * 2 * CHUNKS,)),
            dma((half * 2,)),
            dma((half * 2,)),
            dma((6,)),
            dma((6,)),
            dma((2,)),
            dma((NZ,)),
            dma((NZ,)),
            dma((NZ,)),
            dma((NZ,)),
            dma((NZ // batch,)),
            dma((NZ // batch,)),
            dma((NZ // batch,)),
        ],
        compiler_params=pltpu.CompilerParams(
            collective_id=0, has_side_effects=True, vmem_limit_bytes=VMEM_MIB * 1024 * 1024
        ),
        name="exchange",
    )(tokens, routes.T, weights, keep_mask, factor)
    return out.reshape(count, top, hidden)


def local(tokens, routes, weights, keep_mask, inv_factor):
    p, r, d = weights.shape[1:]
    return exchange(
        tokens, routes, weights.reshape(p * r, d), keep_mask.reshape(p * r, BLK), inv_factor.reshape(BLK, d)
    )


def solution(mesh):
    return jax.shard_map(
        local,
        mesh=mesh,
        in_specs=(
            P(("dp", "expert"), None),
            P(("dp", "expert"), None),
            P("expert", None, "dp", None),
            P("expert", None, "dp", None),
            P("expert", None, None),
        ),
        out_specs=P(("dp", "expert"), None, None),
        check_vma=False,
    )
```

```python
import functools

import jax
import jax.numpy as jnp
from jax import lax
from jax.experimental import pallas as pl
from jax.experimental.pallas import tpu as pltpu
from jax.sharding import PartitionSpec as P

MESH = pl.DeviceIdType.MESH
F32 = jnp.float32
BF16 = jnp.bfloat16
HI = lax.Precision.HIGHEST
BLK = 128
SUB = 16
SLOTS = 8
TILE = 256
CHUNKS = 3
X_STEP = 3
VMEM_MIB = 60
FAR_MET = ()
NY, NZ, NC = 4, 16, 2
ORDER = (4, 1, 3, 5, 7, 8, 6, 2)
EARLY = ((0, True), (1, False))


def iota(shape, dim):
    return lax.broadcasted_iota(jnp.int32, shape, dim)


def dot(a, b, dims, precision=None):
    return lax.dot_general(
        a, b, (dims, ((), ())), precision=precision, preferred_element_type=F32
    )


def prune_body(w_ref, mask_ref, f_ref, out_ref):
    factor = f_ref[:, :BLK]
    row_id = lax.broadcasted_iota(jnp.int32, (BLK, BLK), 0)
    col_id = lax.broadcasted_iota(jnp.int32, (BLK, BLK), 1)
    diagonal = jnp.sum(jnp.where(row_id == col_id, factor, 0.0), axis=1, keepdims=True)
    factor_t = factor.T
    lead = w_ref[:, :BLK].astype(F32).T
    scale = (1 - mask_ref[...]).astype(F32).T / diagonal
    errors, done = [], []
    for start in range(0, BLK, SUB):
        part = lead[:SUB]
        rows = []
        for i in range(SUB):
            g = start + i
            err = part[i : i + 1] * scale[g : g + 1]
            part = part - factor_t[start : start + SUB, g : g + 1] * err
            rows.append(err)
        block = jnp.concatenate(rows, axis=0)
        errors.append(block)
        done.append(part)
        if start + SUB < BLK:
            upd = lax.dot_general(
                factor[start : start + SUB], block, (((0,), (0,)), ((), ())),
                precision=HI, preferred_element_type=F32,
            )
            lead = lead[SUB:] - upd[start + SUB :]
    err_all = jnp.concatenate(errors, axis=0).T
    out_ref[:, :BLK] = jnp.concatenate(done, axis=0).T.astype(out_ref.dtype)
    step = 384
    for at in range(BLK, w_ref.shape[1], step):
        upd = lax.dot_general(
            err_all, f_ref[:, at : at + step], (((1,), (0,)), ((), ())),
            precision=HI, preferred_element_type=F32,
        )
        out_ref[:, at : at + step] = (w_ref[:, at : at + step].astype(F32) - upd).astype(out_ref.dtype)


def exchange_body(nx, tok_in, routes_in, weights_in, mask_in, factor_in, out, tok, weights, mask, factor, pruned,
                  t_up, t_down, rt, packed, rows, whole, batch_rows, hid, back, home, code, last_pick, load_s, ring_s, ring_r,
                  rt_s, rt_r, x_s, x_r, own_s, ys_s, ys_r, zs_s, zs_r, hs_s, hs_r, loc_s):
    tokens, width = tok.shape
    top = routes_in.shape[0]
    slots_all = tokens * top
    own_rows = pruned.shape[0] // 2
    half = NZ // 2
    peers = NY * NC
    owners = NY * NZ * NC
    order = [n for s in ORDER for n in ((s, NZ - s) if s < half else (half, 0))]
    pos_of = {n: p for p, n in enumerate(order)}
    batch = min(4, NZ)
    batches = NZ // batch
    x = lax.axis_index("dp")
    me = lax.axis_index("expert")
    y = me // (NZ * NC)
    z = (me // NC) % NZ
    c = me % NC

    loads = [
        pltpu.make_async_copy(src, dst, load_s.at[i])
        for i, (src, dst) in enumerate(((tok_in, tok), (weights_in, weights), (mask_in, mask), (factor_in, factor)))
    ]
    for copy in loads:
        copy.start()

    def along_z(n):
        return {"expert": (y * NZ + (z + n) % NZ) * NC + c}

    def along_y(q):
        return {"expert": (((y + q // NC) % NY) * NZ + z) * NC + (c + q % NC) % NC}

    def along_x(n):
        return {"dp": (x + n) % nx}

    def mirror(q):
        return ((NY - q // NC) % NY) * NC + q % NC

    def remote(src, dst, s, r, device):
        return pltpu.make_async_remote_copy(
            src_ref=src, dst_ref=dst, send_sem=s, recv_sem=r, device_id=device, device_id_type=MESH
        )

    barrier = pltpu.get_barrier_semaphore()
    met = [along_z(n) for n in (FAR_MET if FAR_MET else sorted({1, NZ - 1}))] + [along_y(q) for q in range(1, peers)]
    if nx > 1:
        met += [along_x(1), along_x(nx - 1)]
    for device in met:
        pl.semaphore_signal(barrier, inc=1, device_id=device, device_id_type=MESH)
    pl.semaphore_wait(barrier, len(met))

    chunk = tokens // CHUNKS

    def ring_rows(way, s, h):
        low, high = h * chunk, h * chunk + chunk
        if s == half:
            low, high = (low, min(high, tokens // 2)) if way == 0 else (max(low, tokens // 2), high)
        return low, high

    def ring_has(way, s, h):
        low, high = ring_rows(way, s, h)
        return s <= half and low < high

    def ring(way, s, h):
        low, high = ring_rows(way, s, h)
        span = pl.ds(low, high - low)
        held = t_up if way == 0 or s == half else t_down
        src = tok.at[span] if s == 1 else (t_up if way == 0 else t_down).at[s - 1, span]
        at = ((s - 1) * 2 + way) * CHUNKS + h
        return remote(src, held.at[s, span], ring_s.at[at], ring_r.at[at], along_z(1 if way == 0 else NZ - 1))

    def names(way, s):
        at = (s - 1) * 2 + way
        src, dst = (NZ - s + 1) % NZ if way == 0 else s - 1, NZ - s if way == 0 else s
        return remote(rt.at[src], rt.at[dst], rt_s.at[at], rt_r.at[at], along_z(1 if way == 0 else NZ - 1))

    def names_has(way, s):
        return s < half or (s == half and way == 0)

    loads[0].wait()
    for h in range(CHUNKS):
        for way in range(2):
            if ring_has(way, 1, h):
                ring(way, 1, h).start()

    rt[0] = jnp.full((top, BLK), -1.0, F32)
    rt[0, :, pl.ds(0, tokens)] = routes_in[...].astype(F32)

    for copy in loads[1:]:
        copy.wait()
    prune_body(weights, mask, factor, pruned)

    x_copies, x_forward = [], []
    span_own = [pl.ds(g * own_rows, own_rows) for g in range(2)]

    def place(g, n):
        return whole.at[g, pl.ds(pl.multiple_of(((x + n) % nx) * own_rows, own_rows), own_rows)]

    for way in range(2):
        if names_has(way, 1):
            names(way, 1).start()
    own_copies = [pltpu.make_async_copy(pruned.at[span_own[g]], place(g, 0), own_s.at[g]) for g in range(2)]
    if nx > 1:
        for i, (n, g) in enumerate(((1, 0), (nx - 1, 1), (1, 1), (nx - 1, 0))):
            copy = remote(pruned.at[span_own[g]], place(g, 0), x_s.at[i], x_r.at[i], along_x(n))
            copy.start()
            x_copies.append(copy)
    for copy in own_copies:
        copy.start()

    def forward_weights():
        if nx > 1:
            x_copies[0].wait_recv()
            x_copies[1].wait_recv()
            for i, (g, n) in enumerate(((0, 1), (1, nx - 1))):
                copy = remote(place(g, nx - n), place(g, nx - n), x_s.at[4 + i], x_r.at[4 + i], along_x(n))
                copy.start()
                x_forward.append(copy)

    def find_code():
        lane = (iota((tokens, BLK), 0) == iota((tokens, BLK), 1)).astype(F32).astype(BF16)
        chosen = dot(lane, rt[0].astype(BF16), ((1,), (1,))).astype(BF16)
        repeat = (iota((slots_all, tokens), 0) // top == iota((slots_all, tokens), 1)).astype(F32).astype(BF16)
        spread = dot(repeat, chosen, ((1,), (0,)))
        mine = iota((slots_all, top), 0) % top == iota((slots_all, top), 1)
        expert_of = jnp.sum(jnp.where(mine, spread, 0.0), axis=1, keepdims=True)
        hot = (expert_of == iota((slots_all, owners), 1).astype(F32)).astype(F32)
        earlier = (iota((slots_all, slots_all), 1) < iota((slots_all, slots_all), 0)).astype(F32).astype(BF16)
        ranks = dot(earlier, hot.astype(BF16), ((1,), (0,)))
        each = iota((1, owners), 1)
        rel = (each // NC % NZ - z + NZ) % NZ
        pos = jnp.zeros_like(rel)
        for n, p in pos_of.items():
            pos = jnp.where(rel == n, p, pos)
        peer = (each // (NZ * NC) - y + NY) % NY * NC + (each % NC - c + NC) % NC
        table = ((pos * peers + peer) * SLOTS).astype(F32)
        code[...] = jnp.broadcast_to(jnp.sum(hot * (ranks + table), axis=1, keepdims=True), code.shape)

    q_id = iota((peers, BLK), 0)
    experts = (((y + q_id // NC) % NY * NZ + z) * NC + (c + q_id % NC) % NC).astype(F32)
    before_token = (iota((BLK, BLK), 0) < iota((BLK, BLK), 1)).astype(F32).astype(BF16)

    def pack(n, block):
        position = pos_of[n]
        named = rt[n]
        hit = jnp.zeros((peers, BLK), F32)
        for k in range(top):
            hit = hit + (named[k : k + 1] == experts).astype(F32)
        rank = dot(hit.astype(BF16), before_token, ((1,), (0,)))
        key = jnp.where(hit > 0, rank, -1.0)
        pick = (key[:, None, :] == iota((peers, SLOTS, BLK), 1).astype(F32)).astype(F32)
        pick = pick.reshape(peers * SLOTS, BLK).astype(BF16)[:, :tokens]
        wide = min(512, width)
        for at in range(0, width, wide):
            cols = pl.ds(at, wide)
            taken = dot(pick, block[:, cols], ((1,), (0,)))
            taken = taken.reshape(peers, SLOTS, wide).astype(BF16)
            packed[position, :, :, cols] = taken
            rows[position, 0, :, cols] = taken[0]

    def to_peer(position, q):
        return remote(packed.at[position, q], rows.at[position, mirror(q)], ys_s.at[position], ys_r.at[position], along_y(q))

    packed_last = []

    def pack_next(n, block):
        pack(n, block)
        hand_out()
        packed_last.append(pos_of[n])

    def hand_out():
        while packed_last:
            position = packed_last.pop()
            for q in range(1, peers):
                to_peer(position, q).start()

    def return_to(n):
        p, q = pos_of[n], pos_of[(NZ - n) % NZ]
        if n == 0:
            return pltpu.make_async_copy(hid.at[p], back.at[p], zs_r.at[p])
        return remote(hid.at[p], back.at[q], zs_s.at[p], zs_r.at[q], along_z(n))

    def straight(n, q):
        p, r = pos_of[n], pos_of[(NZ - n) % NZ]
        device = {"expert": (((y + q // NC) % NY) * NZ + (z + n) % NZ) * NC + (c + q % NC) % NC}
        return remote(hid.at[p, q], home.at[r, mirror(q)], zs_s.at[p], hs_r.at[r], device)

    def multiply(b):
        first = b * batch
        if peers > 1:
            for k in range(batch):
                landed = rows.at[first + k, pl.ds(1, peers - 1)]
                pltpu.make_async_copy(landed, landed, ys_r.at[first + k]).wait()
        count = batch * peers * SLOTS
        batch_rows[...] = rows[pl.ds(first, batch)].astype(F32).reshape(count, width).astype(BF16)
        for at in range(0, whole.shape[1], TILE):
            cols = pl.ds(at, TILE)
            gate = dot(batch_rows[...], whole[0, cols], ((1,), (1,)))
            up = dot(batch_rows[...], whole[1, cols], ((1,), (1,)))
            value = gate / (1.0 + jnp.exp(-gate)) * up
            hid[pl.ds(first, batch), :, :, cols] = value.reshape(batch, peers, SLOTS, TILE).astype(BF16)

    def send_back(b):
        for n in sorted(order[b * batch : (b + 1) * batch], key=lambda n: -min(n, NZ - n)):
            if pos_of[n] < NZ - 2:
                return_to(n).start()
            else:
                for q in range(peers):
                    straight(n, q).start()

    def have_weights():
        for copy in own_copies:
            copy.wait()
        for copy in x_copies[2:] + x_forward:
            copy.wait_recv()

    jobs = {(1, 0): [lambda: pack_next(0, tok)], (1, 1): [find_code]}
    for s in range(1, half if not EARLY else half - 1):
        jobs.setdefault((s + 1, 0), []).append(lambda s=s: pack_next(NZ - s, t_up.at[s]))
        jobs.setdefault((s + 1, 1), []).append(lambda s=s: pack_next(s, t_down.at[s]))
    jobs.setdefault((min(X_STEP, half), 2), []).append(forward_weights)
    if EARLY:
        last = jobs.setdefault((half - 1, CHUNKS - 1), [])
        last += [hand_out, have_weights]
        for b, send in EARLY:
            last.append(lambda b=b: multiply(b))
            if send:
                last.append(lambda b=b: send_back(b))
    for s in range(1, half + 1):
        for h in range(CHUNKS):
            for way in range(2):
                if h == 0 and names_has(way, s):
                    names(way, s).wait_recv()
                    if names_has(way, s + 1):
                        names(way, s + 1).start()
                if ring_has(way, s, h):
                    ring(way, s, h).wait_recv()
                    if ring_has(way, s + 1, h):
                        ring(way, s + 1, h).start()
            for job in jobs.get((s, h), []):
                job()
    for b, send in EARLY:
        if not send:
            send_back(b)
    for n, block in (((NZ - half + 1, 0), (half - 1, 1)) if EARLY else ()):
        pack_next(n, (t_up if block == 0 else t_down).at[n if block else NZ - n])
    pack_next(half, t_up.at[half])
    hand_out()
    if not EARLY:
        have_weights()
    for b in range(batches):
        if b not in [early for early, _ in EARLY]:
            multiply(b)
            send_back(b)

    def drain_outward():
        for s in range(1, half + 1):
            for way in range(2):
                if names_has(way, s):
                    names(way, s).wait_send()
                for h in range(CHUNKS):
                    if ring_has(way, s, h):
                        ring(way, s, h).wait_send()
        for copy in x_copies + x_forward:
            copy.wait_send()
        if peers > 1:
            for p in range(NZ):
                sent = packed.at[p, pl.ds(1, peers - 1)]
                pltpu.make_async_copy(sent, sent, ys_s.at[p]).wait()

    drain_outward()

    def homeward(p, q):
        return remote(back.at[p, q], home.at[p, mirror(q)], hs_s.at[p], hs_r.at[p], along_y(q))

    def stay(p):
        return pltpu.make_async_copy(back.at[p, 0], home.at[p, 0], loc_s.at[p])

    def send_home(p):
        pltpu.make_async_copy(back.at[p], back.at[p], zs_r.at[p]).wait()
        for q in range(1, peers):
            homeward(p, q).start()
        stay(p).start()

    def picks(first, many):
        lanes = iota((slots_all, BLK), 1).astype(F32)
        each = peers * SLOTS
        made = [(code[...] == lanes + float(first * each + at)).astype(F32).astype(BF16) for at in range(0, many * each, BLK)]
        return jnp.concatenate(made, axis=1)[:, : many * each]

    def unpack(first, many, ready):
        pick = last_pick[...] if ready else picks(first, many)
        for p in range(first, first + many):
            if ready:
                pltpu.make_async_copy(home.at[p], home.at[p], hs_r.at[p]).wait()
                continue
            stay(p).wait()
            if peers > 1:
                landed = home.at[p, pl.ds(1, peers - 1)]
                pltpu.make_async_copy(landed, landed, hs_r.at[p]).wait()
        values = home[pl.ds(first, many)].astype(F32).reshape(many * peers * SLOTS, out.shape[1]).astype(BF16)
        for at in range(0, out.shape[1], TILE):
            cols = pl.ds(at, TILE)
            got = dot(pick, values[:, at : at + TILE], ((1,), (0,)))
            if first > 0:
                got = out[:, cols].astype(F32) + got
            out[:, cols] = got.astype(BF16)

    groups = [(first, batch) for first in range(0, NZ - batch, batch)] + [(NZ - 4, 2), (NZ - 2, 2)]
    for i, (first, many) in enumerate(groups):
        for p in sorted(range(first, first + many), key=lambda p: -min(order[p], NZ - order[p])):
            if p < NZ - 2:
                send_home(p)
        if i > 0:
            unpack(*groups[i - 1], False)
    last_pick[...] = picks(*groups[-1])
    for p in range(NZ):
        if order[p] != 0:
            pltpu.make_async_copy(hid.at[p], hid.at[p], zs_s.at[p]).wait()
    unpack(NZ - 2, 2, True)
    if peers > 1:
        for p in range(NZ - 2):
            sent = back.at[p, pl.ds(1, peers - 1)]
            pltpu.make_async_copy(sent, sent, hs_s.at[p]).wait()


def exchange(tokens, routes, weights, keep_mask, factor):
    nx = lax.axis_size("dp")
    count, width = tokens.shape
    top = routes.shape[1]
    own = weights.shape[0]
    hidden = own // 2 * nx
    half, peers = NZ // 2, NY * NC
    batch = min(4, NZ)
    dma = pltpu.SemaphoreType.DMA
    vmem = pltpu.VMEM
    out = pl.pallas_call(
        functools.partial(exchange_body, nx),
        out_shape=jax.ShapeDtypeStruct((count * top, hidden), BF16),
        in_specs=[
            pl.BlockSpec(memory_space=pltpu.HBM),
            pl.BlockSpec(memory_space=pltpu.VMEM),
            pl.BlockSpec(memory_space=pltpu.HBM),
            pl.BlockSpec(memory_space=pltpu.HBM),
            pl.BlockSpec(memory_space=pltpu.HBM),
        ],
        out_specs=pl.BlockSpec(memory_space=pltpu.VMEM),
        scratch_shapes=[
            vmem((count, width), BF16),
            vmem((own, width), BF16),
            vmem((own, BLK), jnp.int32),
            vmem((BLK, width), F32),
            vmem((own, width), BF16),
            vmem((half + 1, count, width), BF16),
            vmem((half, count, width), BF16),
            vmem((NZ, top, BLK), F32),
            vmem((NZ, peers, SLOTS, width), BF16),
            vmem((NZ, peers, SLOTS, width), BF16),
            vmem((2, hidden, width), BF16),
            vmem((batch * peers * SLOTS, width), BF16),
            vmem((NZ, peers, SLOTS, hidden), BF16),
            vmem((NZ, peers, SLOTS, hidden), BF16),
            vmem((NZ, peers, SLOTS, hidden), BF16),
            vmem((count * top, BLK), F32),
            vmem((count * top, 2 * peers * SLOTS), BF16),
            dma((4,)),
            dma((half * 2 * CHUNKS,)),
            dma((half * 2 * CHUNKS,)),
            dma((half * 2,)),
            dma((half * 2,)),
            dma((6,)),
            dma((6,)),
            dma((2,)),
            dma((NZ,)),
            dma((NZ,)),
            dma((NZ,)),
            dma((NZ,)),
            dma((NZ,)),
            dma((NZ,)),
            dma((NZ,)),
        ],
        compiler_params=pltpu.CompilerParams(
            collective_id=0, has_side_effects=True, vmem_limit_bytes=VMEM_MIB * 1024 * 1024
        ),
        name="exchange",
    )(tokens, routes.T, weights, keep_mask, factor)
    return out.reshape(count, top, hidden)


def local(tokens, routes, weights, keep_mask, inv_factor):
    p, r, d = weights.shape[1:]
    return exchange(
        tokens, routes, weights.reshape(p * r, d), keep_mask.reshape(p * r, BLK), inv_factor.reshape(BLK, d)
    )


def solution(mesh):
    return jax.shard_map(
        local,
        mesh=mesh,
        in_specs=(
            P(("dp", "expert"), None),
            P(("dp", "expert"), None),
            P("expert", None, "dp", None),
            P("expert", None, "dp", None),
            P("expert", None, None),
        ),
        out_specs=P(("dp", "expert"), None, None),
        check_vma=False,
    )
```

```python
import functools

import jax
import jax.numpy as jnp
from jax import lax
from jax.experimental import pallas as pl
from jax.experimental.pallas import tpu as pltpu
from jax.sharding import PartitionSpec as P

MESH = pl.DeviceIdType.MESH
F32 = jnp.float32
BF16 = jnp.bfloat16
HI = lax.Precision.HIGHEST
BLK = 128
SUB = 16
SLOTS = 8
TILE = 256
CHUNKS = 3
FINISH_TILES = 2
X_STEP = 3
VMEM_MIB = 60
FAR_MET = ()
NY, NZ, NC = 4, 16, 2
ORDER = (4, 1, 3, 5, 7, 8, 6, 2)
EARLY = ((0, True), (1, False))


def iota(shape, dim):
    return lax.broadcasted_iota(jnp.int32, shape, dim)


def dot(a, b, dims, precision=None):
    return lax.dot_general(
        a, b, (dims, ((), ())), precision=precision, preferred_element_type=F32
    )


def prune_body(w_ref, mask_ref, f_ref, out_ref):
    factor = f_ref[:, :BLK]
    row_id = lax.broadcasted_iota(jnp.int32, (BLK, BLK), 0)
    col_id = lax.broadcasted_iota(jnp.int32, (BLK, BLK), 1)
    diagonal = jnp.sum(jnp.where(row_id == col_id, factor, 0.0), axis=1, keepdims=True)
    factor_t = factor.T
    lead = w_ref[:, :BLK].astype(F32).T
    scale = (1 - mask_ref[...]).astype(F32).T / diagonal
    errors, done = [], []
    for start in range(0, BLK, SUB):
        part = lead[:SUB]
        rows = []
        for i in range(SUB):
            g = start + i
            err = part[i : i + 1] * scale[g : g + 1]
            part = part - factor_t[start : start + SUB, g : g + 1] * err
            rows.append(err)
        block = jnp.concatenate(rows, axis=0)
        errors.append(block)
        done.append(part)
        if start + SUB < BLK:
            upd = lax.dot_general(
                factor[start : start + SUB], block, (((0,), (0,)), ((), ())),
                precision=HI, preferred_element_type=F32,
            )
            lead = lead[SUB:] - upd[start + SUB :]
    err_all = jnp.concatenate(errors, axis=0).T
    out_ref[:, :BLK] = jnp.concatenate(done, axis=0).T.astype(out_ref.dtype)
    step = 384
    for at in range(BLK, w_ref.shape[1], step):
        upd = lax.dot_general(
            err_all, f_ref[:, at : at + step], (((1,), (0,)), ((), ())),
            precision=HI, preferred_element_type=F32,
        )
        out_ref[:, at : at + step] = (w_ref[:, at : at + step].astype(F32) - upd).astype(out_ref.dtype)


def exchange_body(nx, tok_in, routes_in, weights_in, mask_in, factor_in, out_hbm, pick_hbm, last_hbm, tok, weights, mask, factor, pruned,
                  t_up, t_down, rt, packed, rows, whole, batch_rows, hid, back, home, code, out, last_pick, load_s, ring_s, ring_r,
                  rt_s, rt_r, x_s, x_r, own_s, ys_s, ys_r, zs_s, zs_r, hs_s, hs_r, loc_s, out_s):
    tokens, width = tok.shape
    top = routes_in.shape[0]
    slots_all = tokens * top
    own_rows = pruned.shape[0] // 2
    half = NZ // 2
    peers = NY * NC
    owners = NY * NZ * NC
    order = [n for s in ORDER for n in ((s, NZ - s) if s < half else (half, 0))]
    pos_of = {n: p for p, n in enumerate(order)}
    batch = min(4, NZ)
    batches = NZ // batch
    x = lax.axis_index("dp")
    me = lax.axis_index("expert")
    y = me // (NZ * NC)
    z = (me // NC) % NZ
    c = me % NC

    loads = [
        pltpu.make_async_copy(src, dst, load_s.at[i])
        for i, (src, dst) in enumerate(((tok_in, tok), (weights_in, weights), (mask_in, mask), (factor_in, factor)))
    ]
    for copy in loads:
        copy.start()

    def along_z(n):
        return {"expert": (y * NZ + (z + n) % NZ) * NC + c}

    def along_y(q):
        return {"expert": (((y + q // NC) % NY) * NZ + z) * NC + (c + q % NC) % NC}

    def along_x(n):
        return {"dp": (x + n) % nx}

    def mirror(q):
        return ((NY - q // NC) % NY) * NC + q % NC

    def remote(src, dst, s, r, device):
        return pltpu.make_async_remote_copy(
            src_ref=src, dst_ref=dst, send_sem=s, recv_sem=r, device_id=device, device_id_type=MESH
        )

    barrier = pltpu.get_barrier_semaphore()
    met = [along_z(n) for n in (FAR_MET if FAR_MET else sorted({1, NZ - 1}))] + [along_y(q) for q in range(1, peers)]
    if nx > 1:
        met += [along_x(1), along_x(nx - 1)]
    for device in met:
        pl.semaphore_signal(barrier, inc=1, device_id=device, device_id_type=MESH)
    pl.semaphore_wait(barrier, len(met))

    chunk = tokens // CHUNKS

    def ring_rows(way, s, h):
        low, high = h * chunk, h * chunk + chunk
        if s == half:
            low, high = (low, min(high, tokens // 2)) if way == 0 else (max(low, tokens // 2), high)
        return low, high

    def ring_has(way, s, h):
        low, high = ring_rows(way, s, h)
        return s <= half and low < high

    def ring(way, s, h):
        low, high = ring_rows(way, s, h)
        span = pl.ds(low, high - low)
        held = t_up if way == 0 or s == half else t_down
        src = tok.at[span] if s == 1 else (t_up if way == 0 else t_down).at[s - 1, span]
        at = ((s - 1) * 2 + way) * CHUNKS + h
        return remote(src, held.at[s, span], ring_s.at[at], ring_r.at[at], along_z(1 if way == 0 else NZ - 1))

    def names(way, s):
        at = (s - 1) * 2 + way
        src, dst = (NZ - s + 1) % NZ if way == 0 else s - 1, NZ - s if way == 0 else s
        return remote(rt.at[src], rt.at[dst], rt_s.at[at], rt_r.at[at], along_z(1 if way == 0 else NZ - 1))

    def names_has(way, s):
        return s < half or (s == half and way == 0)

    loads[0].wait()
    for h in range(CHUNKS):
        for way in range(2):
            if ring_has(way, 1, h):
                ring(way, 1, h).start()

    rt[0] = jnp.full((top, BLK), -1.0, F32)
    rt[0, :, pl.ds(0, tokens)] = routes_in[...].astype(F32)

    for copy in loads[1:]:
        copy.wait()
    prune_body(weights, mask, factor, pruned)

    x_copies, x_forward = [], []
    span_own = [pl.ds(g * own_rows, own_rows) for g in range(2)]

    def place(g, n):
        return whole.at[g, pl.ds(pl.multiple_of(((x + n) % nx) * own_rows, own_rows), own_rows)]

    for way in range(2):
        if names_has(way, 1):
            names(way, 1).start()
    own_copies = [pltpu.make_async_copy(pruned.at[span_own[g]], place(g, 0), own_s.at[g]) for g in range(2)]
    if nx > 1:
        for i, (n, g) in enumerate(((1, 0), (nx - 1, 1), (1, 1), (nx - 1, 0))):
            copy = remote(pruned.at[span_own[g]], place(g, 0), x_s.at[i], x_r.at[i], along_x(n))
            copy.start()
            x_copies.append(copy)
    for copy in own_copies:
        copy.start()

    def forward_weights():
        if nx > 1:
            x_copies[0].wait_recv()
            x_copies[1].wait_recv()
            for i, (g, n) in enumerate(((0, 1), (1, nx - 1))):
                copy = remote(place(g, nx - n), place(g, nx - n), x_s.at[4 + i], x_r.at[4 + i], along_x(n))
                copy.start()
                x_forward.append(copy)

    def find_code():
        lane = (iota((tokens, BLK), 0) == iota((tokens, BLK), 1)).astype(F32).astype(BF16)
        chosen = dot(lane, rt[0].astype(BF16), ((1,), (1,))).astype(BF16)
        repeat = (iota((slots_all, tokens), 0) // top == iota((slots_all, tokens), 1)).astype(F32).astype(BF16)
        spread = dot(repeat, chosen, ((1,), (0,)))
        mine = iota((slots_all, top), 0) % top == iota((slots_all, top), 1)
        expert_of = jnp.sum(jnp.where(mine, spread, 0.0), axis=1, keepdims=True)
        hot = (expert_of == iota((slots_all, owners), 1).astype(F32)).astype(F32)
        earlier = (iota((slots_all, slots_all), 1) < iota((slots_all, slots_all), 0)).astype(F32).astype(BF16)
        ranks = dot(earlier, hot.astype(BF16), ((1,), (0,)))
        each = iota((1, owners), 1)
        rel = (each // NC % NZ - z + NZ) % NZ
        pos = jnp.zeros_like(rel)
        for n, p in pos_of.items():
            pos = jnp.where(rel == n, p, pos)
        peer = (each // (NZ * NC) - y + NY) % NY * NC + (each % NC - c + NC) % NC
        table = ((pos * peers + peer) * SLOTS).astype(F32)
        code[...] = jnp.broadcast_to(jnp.sum(hot * (ranks + table), axis=1, keepdims=True), code.shape)

    q_id = iota((peers, BLK), 0)
    experts = (((y + q_id // NC) % NY * NZ + z) * NC + (c + q_id % NC) % NC).astype(F32)
    before_token = (iota((BLK, BLK), 0) < iota((BLK, BLK), 1)).astype(F32).astype(BF16)

    def pack(n, block):
        position = pos_of[n]
        named = rt[n]
        hit = jnp.zeros((peers, BLK), F32)
        for k in range(top):
            hit = hit + (named[k : k + 1] == experts).astype(F32)
        rank = dot(hit.astype(BF16), before_token, ((1,), (0,)))
        key = jnp.where(hit > 0, rank, -1.0)
        pick = (key[:, None, :] == iota((peers, SLOTS, BLK), 1).astype(F32)).astype(F32)
        pick = pick.reshape(peers * SLOTS, BLK).astype(BF16)[:, :tokens]
        wide = min(512, width)
        for at in range(0, width, wide):
            cols = pl.ds(at, wide)
            taken = dot(pick, block[:, cols], ((1,), (0,)))
            taken = taken.reshape(peers, SLOTS, wide).astype(BF16)
            packed[position, :, :, cols] = taken
            rows[position, 0, :, cols] = taken[0]

    def to_peer(position, q):
        return remote(packed.at[position, q], rows.at[position, mirror(q)], ys_s.at[position], ys_r.at[position], along_y(q))

    packed_last = []

    def pack_next(n, block):
        pack(n, block)
        hand_out()
        packed_last.append(pos_of[n])

    def hand_out():
        while packed_last:
            position = packed_last.pop()
            for q in range(1, peers):
                to_peer(position, q).start()

    def return_to(n):
        p, q = pos_of[n], pos_of[(NZ - n) % NZ]
        if n == 0:
            return pltpu.make_async_copy(hid.at[p], back.at[p], zs_r.at[p])
        return remote(hid.at[p], back.at[q], zs_s.at[p], zs_r.at[q], along_z(n))

    relayed = NZ - batch

    def straight(n, q):
        p, r = pos_of[n], pos_of[(NZ - n) % NZ]
        device = {"expert": (((y + q // NC) % NY) * NZ + (z + n) % NZ) * NC + (c + q % NC) % NC}
        return remote(hid.at[p, q], last_hbm.at[r - relayed, mirror(q)], zs_s.at[p], hs_r.at[r], device)

    def multiply(b):
        first = b * batch
        if peers > 1:
            for k in range(batch):
                landed = rows.at[first + k, pl.ds(1, peers - 1)]
                pltpu.make_async_copy(landed, landed, ys_r.at[first + k]).wait()
        count = batch * peers * SLOTS
        batch_rows[...] = rows[pl.ds(first, batch)].astype(F32).reshape(count, width).astype(BF16)
        for at in range(0, whole.shape[1], TILE):
            cols = pl.ds(at, TILE)
            gate = dot(batch_rows[...], whole[0, cols], ((1,), (1,)))
            up = dot(batch_rows[...], whole[1, cols], ((1,), (1,)))
            value = gate / (1.0 + jnp.exp(-gate)) * up
            hid[pl.ds(first, batch), :, :, cols] = value.reshape(batch, peers, SLOTS, TILE).astype(BF16)

    def send_back(b):
        for n in sorted(order[b * batch : (b + 1) * batch], key=lambda n: -min(n, NZ - n)):
            if pos_of[n] < relayed:
                return_to(n).start()
            else:
                for q in range(peers):
                    straight(n, q).start()

    def have_weights():
        for copy in own_copies:
            copy.wait()
        for copy in x_copies[2:] + x_forward:
            copy.wait_recv()

    jobs = {(1, 0): [lambda: pack_next(0, tok)], (1, 1): [find_code]}
    for s in range(1, half if not EARLY else half - 1):
        jobs.setdefault((s + 1, 0), []).append(lambda s=s: pack_next(NZ - s, t_up.at[s]))
        jobs.setdefault((s + 1, 1), []).append(lambda s=s: pack_next(s, t_down.at[s]))
    jobs.setdefault((min(X_STEP, half), 2), []).append(forward_weights)
    if EARLY:
        last = jobs.setdefault((half - 1, CHUNKS - 1), [])
        last += [hand_out, have_weights]
        for b, send in EARLY:
            last.append(lambda b=b: multiply(b))
            if send:
                last.append(lambda b=b: send_back(b))
    for s in range(1, half + 1):
        for h in range(CHUNKS):
            for way in range(2):
                if h == 0 and names_has(way, s):
                    names(way, s).wait_recv()
                    if names_has(way, s + 1):
                        names(way, s + 1).start()
                if ring_has(way, s, h):
                    ring(way, s, h).wait_recv()
                    if ring_has(way, s + 1, h):
                        ring(way, s + 1, h).start()
            for job in jobs.get((s, h), []):
                job()
    for b, send in EARLY:
        if not send:
            send_back(b)
    for n, block in (((NZ - half + 1, 0), (half - 1, 1)) if EARLY else ()):
        pack_next(n, (t_up if block == 0 else t_down).at[n if block else NZ - n])
    pack_next(half, t_up.at[half])
    hand_out()
    if not EARLY:
        have_weights()
    for b in range(batches):
        if b not in [early for early, _ in EARLY]:
            multiply(b)
            send_back(b)

    def drain_outward():
        for s in range(1, half + 1):
            for way in range(2):
                if names_has(way, s):
                    names(way, s).wait_send()
                for h in range(CHUNKS):
                    if ring_has(way, s, h):
                        ring(way, s, h).wait_send()
        for copy in x_copies + x_forward:
            copy.wait_send()
        if peers > 1:
            for p in range(NZ):
                sent = packed.at[p, pl.ds(1, peers - 1)]
                pltpu.make_async_copy(sent, sent, ys_s.at[p]).wait()

    drain_outward()

    def homeward(p, q):
        return remote(back.at[p, q], home.at[p, mirror(q)], hs_s.at[p], hs_r.at[p], along_y(q))

    def stay(p):
        return pltpu.make_async_copy(back.at[p, 0], home.at[p, 0], loc_s.at[p])

    def send_home(p):
        pltpu.make_async_copy(back.at[p], back.at[p], zs_r.at[p]).wait()
        for q in range(1, peers):
            homeward(p, q).start()
        stay(p).start()

    def picks(first, many):
        lanes = iota((slots_all, BLK), 1).astype(F32)
        each = peers * SLOTS
        made = [(code[...] == lanes + float(first * each + at)).astype(F32).astype(BF16) for at in range(0, many * each, BLK)]
        return jnp.concatenate(made, axis=1)[:, : many * each]

    def unpack(first):
        pick = picks(first, batch)
        for p in range(first, first + batch):
            stay(p).wait()
            if peers > 1:
                landed = home.at[p, pl.ds(1, peers - 1)]
                pltpu.make_async_copy(landed, landed, hs_r.at[p]).wait()
        values = flat(home[pl.ds(first, batch)])
        for at in range(0, out.shape[1], TILE):
            cols = pl.ds(at, TILE)
            got = dot(pick, values[:, at : at + TILE], ((1,), (0,)))
            if first > 0:
                got = out[:, cols].astype(F32) + got
            out[:, cols] = got.astype(BF16)

    last_pick[...] = picks(relayed, batch)
    pick_out = pltpu.make_async_copy(last_pick, pick_hbm, out_s.at[0])
    pick_out.start()
    for first in range(0, relayed, batch):
        for p in sorted(range(first, first + batch), key=lambda p: -min(order[p], NZ - order[p])):
            send_home(p)
        if first > 0:
            unpack(first - batch)
    unpack(relayed - batch)
    total_out = pltpu.make_async_copy(out, out_hbm, out_s.at[1])
    total_out.start()
    for p in range(NZ):
        if order[p] != 0:
            pltpu.make_async_copy(hid.at[p], hid.at[p], zs_s.at[p]).wait()
    if peers > 1:
        for p in range(relayed):
            sent = back.at[p, pl.ds(1, peers - 1)]
            pltpu.make_async_copy(sent, sent, hs_s.at[p]).wait()
    pick_out.wait()
    total_out.wait()
    for k in range(batch):
        pltpu.make_async_copy(last_hbm.at[k], last_hbm.at[k], hs_r.at[relayed + k]).wait()


def flat(values):
    return values.astype(F32).reshape(-1, values.shape[-1]).astype(BF16)


def finish_body(partial, pick, last, out):
    got = dot(pick[...], flat(last[...]), ((1,), (0,)))
    out[...] = (partial[...].astype(F32) + got).astype(BF16)


def finish(partial, pick, last):
    rows, hidden = partial.shape
    tile = rows // FINISH_TILES
    return pl.pallas_call(
        finish_body,
        grid=(FINISH_TILES,),
        out_shape=jax.ShapeDtypeStruct((rows, hidden), BF16),
        in_specs=[
            pl.BlockSpec((tile, hidden), lambda i: (i, 0)),
            pl.BlockSpec((tile, pick.shape[1]), lambda i: (i, 0)),
            pl.BlockSpec(last.shape, lambda i: (0, 0, 0, 0)),
        ],
        out_specs=pl.BlockSpec((tile, hidden), lambda i: (i, 0)),
        name="finish",
    )(partial, pick, last)


def exchange(tokens, routes, weights, keep_mask, factor):
    nx = lax.axis_size("dp")
    count, width = tokens.shape
    top = routes.shape[1]
    own = weights.shape[0]
    hidden = own // 2 * nx
    half, peers = NZ // 2, NY * NC
    batch = min(4, NZ)
    dma = pltpu.SemaphoreType.DMA
    vmem = pltpu.VMEM
    out = pl.pallas_call(
        functools.partial(exchange_body, nx),
        out_shape=[
            jax.ShapeDtypeStruct((count * top, hidden), BF16),
            jax.ShapeDtypeStruct((count * top, batch * peers * SLOTS), BF16),
            jax.ShapeDtypeStruct((batch, peers, SLOTS, hidden), BF16),
        ],
        in_specs=[
            pl.BlockSpec(memory_space=pltpu.HBM),
            pl.BlockSpec(memory_space=pltpu.VMEM),
            pl.BlockSpec(memory_space=pltpu.HBM),
            pl.BlockSpec(memory_space=pltpu.HBM),
            pl.BlockSpec(memory_space=pltpu.HBM),
        ],
        out_specs=[pl.BlockSpec(memory_space=pltpu.HBM)] * 3,
        scratch_shapes=[
            vmem((count, width), BF16),
            vmem((own, width), BF16),
            vmem((own, BLK), jnp.int32),
            vmem((BLK, width), F32),
            vmem((own, width), BF16),
            vmem((half + 1, count, width), BF16),
            vmem((half, count, width), BF16),
            vmem((NZ, top, BLK), F32),
            vmem((NZ, peers, SLOTS, width), BF16),
            vmem((NZ, peers, SLOTS, width), BF16),
            vmem((2, hidden, width), BF16),
            vmem((batch * peers * SLOTS, width), BF16),
            vmem((NZ, peers, SLOTS, hidden), BF16),
            vmem((NZ, peers, SLOTS, hidden), BF16),
            vmem((NZ, peers, SLOTS, hidden), BF16),
            vmem((count * top, BLK), F32),
            vmem((count * top, hidden), BF16),
            vmem((count * top, batch * peers * SLOTS), BF16),
            dma((4,)),
            dma((half * 2 * CHUNKS,)),
            dma((half * 2 * CHUNKS,)),
            dma((half * 2,)),
            dma((half * 2,)),
            dma((6,)),
            dma((6,)),
            dma((2,)),
            dma((NZ,)),
            dma((NZ,)),
            dma((NZ,)),
            dma((NZ,)),
            dma((NZ,)),
            dma((NZ,)),
            dma((NZ,)),
            dma((2,)),
        ],
        compiler_params=pltpu.CompilerParams(
            collective_id=0, has_side_effects=True, vmem_limit_bytes=VMEM_MIB * 1024 * 1024
        ),
        name="exchange",
    )(tokens, routes.T, weights, keep_mask, factor)
    return finish(*out).reshape(count, top, hidden)


def local(tokens, routes, weights, keep_mask, inv_factor):
    p, r, d = weights.shape[1:]
    return exchange(
        tokens, routes, weights.reshape(p * r, d), keep_mask.reshape(p * r, BLK), inv_factor.reshape(BLK, d)
    )


def solution(mesh):
    return jax.shard_map(
        local,
        mesh=mesh,
        in_specs=(
            P(("dp", "expert"), None),
            P(("dp", "expert"), None),
            P("expert", None, "dp", None),
            P("expert", None, "dp", None),
            P("expert", None, None),
        ),
        out_specs=P(("dp", "expert"), None, None),
        check_vma=False,
    )
```

```python
import functools

import jax
import jax.numpy as jnp
from jax import lax
from jax.experimental import pallas as pl
from jax.experimental.pallas import tpu as pltpu
from jax.sharding import PartitionSpec as P

MESH = pl.DeviceIdType.MESH
F32 = jnp.float32
BF16 = jnp.bfloat16
HI = lax.Precision.HIGHEST
BLK = 128
SUB = 16
SLOTS = 8
TILE = 256
CHUNKS = 3
FINISH_TILES = 2
X_STEP = 3
VMEM_MIB = 60
FAR_MET = ()
NY, NZ, NC = 4, 16, 2
ORDER = (2, 1, 3, 5, 7, 8, 6, 4)
EARLY = ((0, True), (1, False))


def iota(shape, dim):
    return lax.broadcasted_iota(jnp.int32, shape, dim)


def dot(a, b, dims, precision=None):
    return lax.dot_general(
        a, b, (dims, ((), ())), precision=precision, preferred_element_type=F32
    )


def prune_body(w_ref, mask_ref, f_ref, out_ref):
    factor = f_ref[:, :BLK]
    row_id = lax.broadcasted_iota(jnp.int32, (BLK, BLK), 0)
    col_id = lax.broadcasted_iota(jnp.int32, (BLK, BLK), 1)
    diagonal = jnp.sum(jnp.where(row_id == col_id, factor, 0.0), axis=1, keepdims=True)
    factor_t = factor.T
    lead = w_ref[:, :BLK].astype(F32).T
    scale = (1 - mask_ref[...]).astype(F32).T / diagonal
    errors, done = [], []
    for start in range(0, BLK, SUB):
        part = lead[:SUB]
        rows = []
        for i in range(SUB):
            g = start + i
            err = part[i : i + 1] * scale[g : g + 1]
            part = part - factor_t[start : start + SUB, g : g + 1] * err
            rows.append(err)
        block = jnp.concatenate(rows, axis=0)
        errors.append(block)
        done.append(part)
        if start + SUB < BLK:
            upd = lax.dot_general(
                factor[start : start + SUB], block, (((0,), (0,)), ((), ())),
                precision=HI, preferred_element_type=F32,
            )
            lead = lead[SUB:] - upd[start + SUB :]
    err_all = jnp.concatenate(errors, axis=0).T
    out_ref[:, :BLK] = jnp.concatenate(done, axis=0).T.astype(out_ref.dtype)
    step = 384
    for at in range(BLK, w_ref.shape[1], step):
        upd = lax.dot_general(
            err_all, f_ref[:, at : at + step], (((1,), (0,)), ((), ())),
            precision=HI, preferred_element_type=F32,
        )
        out_ref[:, at : at + step] = (w_ref[:, at : at + step].astype(F32) - upd).astype(out_ref.dtype)


def exchange_body(nx, tok_in, routes_in, weights_in, mask_in, factor_in, out_hbm, pick_hbm, last_hbm, tok, weights, mask, factor, pruned,
                  t_up, t_down, rt, packed, rows, whole, batch_rows, hid, back, home, code, out, last_pick, load_s, ring_s, ring_r,
                  rt_s, rt_r, x_s, x_r, own_s, ys_s, ys_r, zs_s, zs_r, hs_s, hs_r, loc_s, out_s):
    tokens, width = tok.shape
    top = routes_in.shape[0]
    slots_all = tokens * top
    own_rows = pruned.shape[0] // 2
    half = NZ // 2
    peers = NY * NC
    owners = NY * NZ * NC
    order = [n for s in ORDER for n in ((s, NZ - s) if s < half else (half, 0))]
    pos_of = {n: p for p, n in enumerate(order)}
    batch = min(4, NZ)
    batches = NZ // batch
    x = lax.axis_index("dp")
    me = lax.axis_index("expert")
    y = me // (NZ * NC)
    z = (me // NC) % NZ
    c = me % NC

    loads = [
        pltpu.make_async_copy(src, dst, load_s.at[i])
        for i, (src, dst) in enumerate(((tok_in, tok), (weights_in, weights), (mask_in, mask), (factor_in, factor)))
    ]
    for copy in loads:
        copy.start()

    def along_z(n):
        return {"expert": (y * NZ + (z + n) % NZ) * NC + c}

    def along_y(q):
        return {"expert": (((y + q // NC) % NY) * NZ + z) * NC + (c + q % NC) % NC}

    def along_x(n):
        return {"dp": (x + n) % nx}

    def mirror(q):
        return ((NY - q // NC) % NY) * NC + q % NC

    def remote(src, dst, s, r, device):
        return pltpu.make_async_remote_copy(
            src_ref=src, dst_ref=dst, send_sem=s, recv_sem=r, device_id=device, device_id_type=MESH
        )

    barrier = pltpu.get_barrier_semaphore()
    met = [along_z(n) for n in (FAR_MET if FAR_MET else sorted({1, NZ - 1}))] + [along_y(q) for q in range(1, peers)]
    if nx > 1:
        met += [along_x(1), along_x(nx - 1)]
    for device in met:
        pl.semaphore_signal(barrier, inc=1, device_id=device, device_id_type=MESH)
    pl.semaphore_wait(barrier, len(met))

    chunk = tokens // CHUNKS

    def ring_rows(way, s, h):
        low, high = h * chunk, h * chunk + chunk
        if s == half:
            low, high = (low, min(high, tokens // 2)) if way == 0 else (max(low, tokens // 2), high)
        return low, high

    def ring_has(way, s, h):
        low, high = ring_rows(way, s, h)
        return s <= half and low < high

    def ring(way, s, h):
        low, high = ring_rows(way, s, h)
        span = pl.ds(low, high - low)
        held = t_up if way == 0 or s == half else t_down
        src = tok.at[span] if s == 1 else (t_up if way == 0 else t_down).at[s - 1, span]
        at = ((s - 1) * 2 + way) * CHUNKS + h
        return remote(src, held.at[s, span], ring_s.at[at], ring_r.at[at], along_z(1 if way == 0 else NZ - 1))

    def names(way, s):
        at = (s - 1) * 2 + way
        src, dst = (NZ - s + 1) % NZ if way == 0 else s - 1, NZ - s if way == 0 else s
        return remote(rt.at[src], rt.at[dst], rt_s.at[at], rt_r.at[at], along_z(1 if way == 0 else NZ - 1))

    def names_has(way, s):
        return s < half or (s == half and way == 0)

    loads[0].wait()
    for h in range(CHUNKS):
        for way in range(2):
            if ring_has(way, 1, h):
                ring(way, 1, h).start()

    rt[0] = jnp.full((top, BLK), -1.0, F32)
    rt[0, :, pl.ds(0, tokens)] = routes_in[...].astype(F32)

    for copy in loads[1:]:
        copy.wait()
    prune_body(weights, mask, factor, pruned)

    x_copies, x_forward = [], []
    span_own = [pl.ds(g * own_rows, own_rows) for g in range(2)]

    def place(g, n):
        return whole.at[g, pl.ds(pl.multiple_of(((x + n) % nx) * own_rows, own_rows), own_rows)]

    for way in range(2):
        if names_has(way, 1):
            names(way, 1).start()
    own_copies = [pltpu.make_async_copy(pruned.at[span_own[g]], place(g, 0), own_s.at[g]) for g in range(2)]
    if nx > 1:
        for i, (n, g) in enumerate(((1, 0), (nx - 1, 1), (1, 1), (nx - 1, 0))):
            copy = remote(pruned.at[span_own[g]], place(g, 0), x_s.at[i], x_r.at[i], along_x(n))
            copy.start()
            x_copies.append(copy)
    for copy in own_copies:
        copy.start()

    def forward_weights():
        if nx > 1:
            x_copies[0].wait_recv()
            x_copies[1].wait_recv()
            for i, (g, n) in enumerate(((0, 1), (1, nx - 1))):
                copy = remote(place(g, nx - n), place(g, nx - n), x_s.at[4 + i], x_r.at[4 + i], along_x(n))
                copy.start()
                x_forward.append(copy)

    def find_code():
        lane = (iota((tokens, BLK), 0) == iota((tokens, BLK), 1)).astype(F32).astype(BF16)
        chosen = dot(lane, rt[0].astype(BF16), ((1,), (1,))).astype(BF16)
        repeat = (iota((slots_all, tokens), 0) // top == iota((slots_all, tokens), 1)).astype(F32).astype(BF16)
        spread = dot(repeat, chosen, ((1,), (0,)))
        mine = iota((slots_all, top), 0) % top == iota((slots_all, top), 1)
        expert_of = jnp.sum(jnp.where(mine, spread, 0.0), axis=1, keepdims=True)
        hot = (expert_of == iota((slots_all, owners), 1).astype(F32)).astype(F32)
        earlier = (iota((slots_all, slots_all), 1) < iota((slots_all, slots_all), 0)).astype(F32).astype(BF16)
        ranks = dot(earlier, hot.astype(BF16), ((1,), (0,)))
        each = iota((1, owners), 1)
        rel = (each // NC % NZ - z + NZ) % NZ
        pos = jnp.zeros_like(rel)
        for n, p in pos_of.items():
            pos = jnp.where(rel == n, p, pos)
        peer = (each // (NZ * NC) - y + NY) % NY * NC + (each % NC - c + NC) % NC
        table = ((pos * peers + peer) * SLOTS).astype(F32)
        code[...] = jnp.broadcast_to(jnp.sum(hot * (ranks + table), axis=1, keepdims=True), code.shape)

    q_id = iota((peers, BLK), 0)
    experts = (((y + q_id // NC) % NY * NZ + z) * NC + (c + q_id % NC) % NC).astype(F32)
    before_token = (iota((BLK, BLK), 0) < iota((BLK, BLK), 1)).astype(F32).astype(BF16)

    def pack(n, block):
        position = pos_of[n]
        named = rt[n]
        hit = jnp.zeros((peers, BLK), F32)
        for k in range(top):
            hit = hit + (named[k : k + 1] == experts).astype(F32)
        rank = dot(hit.astype(BF16), before_token, ((1,), (0,)))
        key = jnp.where(hit > 0, rank, -1.0)
        pick = (key[:, None, :] == iota((peers, SLOTS, BLK), 1).astype(F32)).astype(F32)
        pick = pick.reshape(peers * SLOTS, BLK).astype(BF16)[:, :tokens]
        wide = min(512, width)
        for at in range(0, width, wide):
            cols = pl.ds(at, wide)
            taken = dot(pick, block[:, cols], ((1,), (0,)))
            taken = taken.reshape(peers, SLOTS, wide).astype(BF16)
            packed[position, :, :, cols] = taken
            rows[position, 0, :, cols] = taken[0]

    def to_peer(position, q):
        return remote(packed.at[position, q], rows.at[position, mirror(q)], ys_s.at[position], ys_r.at[position], along_y(q))

    packed_last = []

    def pack_next(n, block):
        pack(n, block)
        hand_out()
        packed_last.append(pos_of[n])

    def hand_out():
        while packed_last:
            position = packed_last.pop()
            for q in range(1, peers):
                to_peer(position, q).start()

    def return_to(n):
        p, q = pos_of[n], pos_of[(NZ - n) % NZ]
        if n == 0:
            return pltpu.make_async_copy(hid.at[p], back.at[p], zs_r.at[p])
        return remote(hid.at[p], back.at[q], zs_s.at[p], zs_r.at[q], along_z(n))

    relayed = NZ - batch

    def straight(n, q):
        p, r = pos_of[n], pos_of[(NZ - n) % NZ]
        device = {"expert": (((y + q // NC) % NY) * NZ + (z + n) % NZ) * NC + (c + q % NC) % NC}
        return remote(hid.at[p, q], last_hbm.at[r - relayed, mirror(q)], zs_s.at[p], hs_r.at[r], device)

    def multiply(b):
        first = b * batch
        if peers > 1:
            for k in range(batch):
                landed = rows.at[first + k, pl.ds(1, peers - 1)]
                pltpu.make_async_copy(landed, landed, ys_r.at[first + k]).wait()
        count = batch * peers * SLOTS
        batch_rows[...] = rows[pl.ds(first, batch)].astype(F32).reshape(count, width).astype(BF16)
        for at in range(0, whole.shape[1], TILE):
            cols = pl.ds(at, TILE)
            gate = dot(batch_rows[...], whole[0, cols], ((1,), (1,)))
            up = dot(batch_rows[...], whole[1, cols], ((1,), (1,)))
            value = gate / (1.0 + jnp.exp(-gate)) * up
            hid[pl.ds(first, batch), :, :, cols] = value.reshape(batch, peers, SLOTS, TILE).astype(BF16)

    def send_back(b):
        for n in sorted(order[b * batch : (b + 1) * batch], key=lambda n: -min(n, NZ - n)):
            if pos_of[n] < relayed:
                return_to(n).start()
            else:
                for q in range(peers):
                    straight(n, q).start()

    def have_weights():
        for copy in own_copies:
            copy.wait()
        for copy in x_copies[2:] + x_forward:
            copy.wait_recv()

    jobs = {(1, 0): [lambda: pack_next(0, tok)], (1, 1): [find_code]}
    for s in range(1, half if not EARLY else half - 1):
        jobs.setdefault((s + 1, 0), []).append(lambda s=s: pack_next(NZ - s, t_up.at[s]))
        jobs.setdefault((s + 1, 1), []).append(lambda s=s: pack_next(s, t_down.at[s]))
    jobs.setdefault((min(X_STEP, half), 2), []).append(forward_weights)
    if EARLY:
        last = jobs.setdefault((half - 1, CHUNKS - 1), [])
        last += [hand_out, have_weights]
        for b, send in EARLY:
            last.append(lambda b=b: multiply(b))
            if send:
                last.append(lambda b=b: send_back(b))
    for s in range(1, half + 1):
        for h in range(CHUNKS):
            for way in range(2):
                if h == 0 and names_has(way, s):
                    names(way, s).wait_recv()
                    if names_has(way, s + 1):
                        names(way, s + 1).start()
                if ring_has(way, s, h):
                    ring(way, s, h).wait_recv()
                    if ring_has(way, s + 1, h):
                        ring(way, s + 1, h).start()
            for job in jobs.get((s, h), []):
                job()
    for b, send in EARLY:
        if not send:
            send_back(b)
    for n, block in (((NZ - half + 1, 0), (half - 1, 1)) if EARLY else ()):
        pack_next(n, (t_up if block == 0 else t_down).at[n if block else NZ - n])
    pack_next(half, t_up.at[half])
    hand_out()
    if not EARLY:
        have_weights()
    for b in range(batches):
        if b not in [early for early, _ in EARLY]:
            multiply(b)
            send_back(b)

    def drain_outward():
        for s in range(1, half + 1):
            for way in range(2):
                if names_has(way, s):
                    names(way, s).wait_send()
                for h in range(CHUNKS):
                    if ring_has(way, s, h):
                        ring(way, s, h).wait_send()
        for copy in x_copies + x_forward:
            copy.wait_send()
        if peers > 1:
            for p in range(NZ):
                sent = packed.at[p, pl.ds(1, peers - 1)]
                pltpu.make_async_copy(sent, sent, ys_s.at[p]).wait()

    drain_outward()

    def homeward(p, q):
        return remote(back.at[p, q], home.at[p, mirror(q)], hs_s.at[p], hs_r.at[p], along_y(q))

    def stay(p):
        return pltpu.make_async_copy(back.at[p, 0], home.at[p, 0], loc_s.at[p])

    def send_home(p):
        pltpu.make_async_copy(back.at[p], back.at[p], zs_r.at[p]).wait()
        for q in range(1, peers):
            homeward(p, q).start()
        stay(p).start()

    def picks(first, many):
        lanes = iota((slots_all, BLK), 1).astype(F32)
        each = peers * SLOTS
        made = [(code[...] == lanes + float(first * each + at)).astype(F32).astype(BF16) for at in range(0, many * each, BLK)]
        return jnp.concatenate(made, axis=1)[:, : many * each]

    def unpack(first):
        pick = picks(first, batch)
        for p in range(first, first + batch):
            stay(p).wait()
            if peers > 1:
                landed = home.at[p, pl.ds(1, peers - 1)]
                pltpu.make_async_copy(landed, landed, hs_r.at[p]).wait()
        values = flat(home[pl.ds(first, batch)])
        for at in range(0, out.shape[1], TILE):
            cols = pl.ds(at, TILE)
            got = dot(pick, values[:, at : at + TILE], ((1,), (0,)))
            if first > 0:
                got = out[:, cols].astype(F32) + got
            out[:, cols] = got.astype(BF16)

    last_pick[...] = picks(relayed, batch)
    pick_out = pltpu.make_async_copy(last_pick, pick_hbm, out_s.at[0])
    pick_out.start()
    for first in range(0, relayed, batch):
        for p in sorted(range(first, first + batch), key=lambda p: -min(order[p], NZ - order[p])):
            send_home(p)
        if first > 0:
            unpack(first - batch)
    unpack(relayed - batch)
    total_out = pltpu.make_async_copy(out, out_hbm, out_s.at[1])
    total_out.start()
    for p in range(NZ):
        if order[p] != 0:
            pltpu.make_async_copy(hid.at[p], hid.at[p], zs_s.at[p]).wait()
    if peers > 1:
        for p in range(relayed):
            sent = back.at[p, pl.ds(1, peers - 1)]
            pltpu.make_async_copy(sent, sent, hs_s.at[p]).wait()
    pick_out.wait()
    total_out.wait()
    for k in range(batch):
        pltpu.make_async_copy(last_hbm.at[k], last_hbm.at[k], hs_r.at[relayed + k]).wait()


def flat(values):
    return values.astype(F32).reshape(-1, values.shape[-1]).astype(BF16)


def finish_body(partial, pick, last, out):
    got = dot(pick[...], flat(last[...]), ((1,), (0,)))
    out[...] = (partial[...].astype(F32) + got).astype(BF16)


def finish(partial, pick, last):
    rows, hidden = partial.shape
    tile = rows // FINISH_TILES
    return pl.pallas_call(
        finish_body,
        grid=(FINISH_TILES,),
        out_shape=jax.ShapeDtypeStruct((rows, hidden), BF16),
        in_specs=[
            pl.BlockSpec((tile, hidden), lambda i: (i, 0)),
            pl.BlockSpec((tile, pick.shape[1]), lambda i: (i, 0)),
            pl.BlockSpec(last.shape, lambda i: (0, 0, 0, 0)),
        ],
        out_specs=pl.BlockSpec((tile, hidden), lambda i: (i, 0)),
        name="finish",
    )(partial, pick, last)


def exchange(tokens, routes, weights, keep_mask, factor):
    nx = lax.axis_size("dp")
    count, width = tokens.shape
    top = routes.shape[1]
    own = weights.shape[0]
    hidden = own // 2 * nx
    half, peers = NZ // 2, NY * NC
    batch = min(4, NZ)
    dma = pltpu.SemaphoreType.DMA
    vmem = pltpu.VMEM
    out = pl.pallas_call(
        functools.partial(exchange_body, nx),
        out_shape=[
            jax.ShapeDtypeStruct((count * top, hidden), BF16),
            jax.ShapeDtypeStruct((count * top, batch * peers * SLOTS), BF16),
            jax.ShapeDtypeStruct((batch, peers, SLOTS, hidden), BF16),
        ],
        in_specs=[
            pl.BlockSpec(memory_space=pltpu.HBM),
            pl.BlockSpec(memory_space=pltpu.VMEM),
            pl.BlockSpec(memory_space=pltpu.HBM),
            pl.BlockSpec(memory_space=pltpu.HBM),
            pl.BlockSpec(memory_space=pltpu.HBM),
        ],
        out_specs=[pl.BlockSpec(memory_space=pltpu.HBM)] * 3,
        scratch_shapes=[
            vmem((count, width), BF16),
            vmem((own, width), BF16),
            vmem((own, BLK), jnp.int32),
            vmem((BLK, width), F32),
            vmem((own, width), BF16),
            vmem((half + 1, count, width), BF16),
            vmem((half, count, width), BF16),
            vmem((NZ, top, BLK), F32),
            vmem((NZ, peers, SLOTS, width), BF16),
            vmem((NZ, peers, SLOTS, width), BF16),
            vmem((2, hidden, width), BF16),
            vmem((batch * peers * SLOTS, width), BF16),
            vmem((NZ, peers, SLOTS, hidden), BF16),
            vmem((NZ, peers, SLOTS, hidden), BF16),
            vmem((NZ, peers, SLOTS, hidden), BF16),
            vmem((count * top, BLK), F32),
            vmem((count * top, hidden), BF16),
            vmem((count * top, batch * peers * SLOTS), BF16),
            dma((4,)),
            dma((half * 2 * CHUNKS,)),
            dma((half * 2 * CHUNKS,)),
            dma((half * 2,)),
            dma((half * 2,)),
            dma((6,)),
            dma((6,)),
            dma((2,)),
            dma((NZ,)),
            dma((NZ,)),
            dma((NZ,)),
            dma((NZ,)),
            dma((NZ,)),
            dma((NZ,)),
            dma((NZ,)),
            dma((2,)),
        ],
        compiler_params=pltpu.CompilerParams(
            collective_id=0, has_side_effects=True, vmem_limit_bytes=VMEM_MIB * 1024 * 1024
        ),
        name="exchange",
    )(tokens, routes.T, weights, keep_mask, factor)
    return finish(*out).reshape(count, top, hidden)


def local(tokens, routes, weights, keep_mask, inv_factor):
    p, r, d = weights.shape[1:]
    return exchange(
        tokens, routes, weights.reshape(p * r, d), keep_mask.reshape(p * r, BLK), inv_factor.reshape(BLK, d)
    )


def solution(mesh):
    return jax.shard_map(
        local,
        mesh=mesh,
        in_specs=(
            P(("dp", "expert"), None),
            P(("dp", "expert"), None),
            P("expert", None, "dp", None),
            P("expert", None, "dp", None),
            P("expert", None, None),
        ),
        out_specs=P(("dp", "expert"), None, None),
        check_vma=False,
    )
```
